8 devices in a mesh: replica: 2 (over z, y), dp: 4 (over x, core).
Axes of the slice: x: 2, y: 2, z: 1, core: 2. Of those that a mesh axis runs over, the one named last changes fastest.
Arguments:
- x: bfloat16 [1024, 256], P(('replica', 'dp')), parts along dimension 0
- lengths: int32 [1024], P(('replica', 'dp')), parts along dimension 0
- cache: bfloat16 [2, 1024, 512, 576], P(None, ('replica', 'dp')), parts along dimension 1
- w_q: bfloat16 [2, 256, 1152], replicated
- w_o: bfloat16 [2, 1024, 256], replicated
- expert_ids: int32 [2, 1024, 6], P(None, ('replica', 'dp')), parts along dimension 1
- slots: int32 [2, 1024, 6], P(None, ('replica', 'dp')), parts along dimension 1
- route_w: float32 [2, 1024, 6], P(None, ('replica', 'dp')), parts along dimension 1
- w1_exp: bfloat16 [2, 64, 256, 176], P(None, 'dp')
- w3_exp: bfloat16 [2, 64, 256, 176], P(None, 'dp')
- w2_exp: bfloat16 [2, 64, 176, 256], P(None, 'dp')
- w1_sh: bfloat16 [2, 256, 352], P(None, None, 'dp')
- w3_sh: bfloat16 [2, 256, 352], P(None, None, 'dp')
- w2_sh: bfloat16 [2, 352, 256], P(None, 'dp')
Outputs:
- output: bfloat16 [1024, 256], P(('replica', 'dp')), parts along dimension 0
There are 2 independent parts. The reference program is written for one: setup_inputs(seed, part) draws one part's arguments, and reference() takes and returns one part's arrays. A program takes and returns all parts, laid end to end along the dimension named above; an argument that names none is the same for every part.
All inputs are finite; a program needn't handle non-finite values.
Results may differ from the reference program's by a relative error of at most 0.02.
Values are sent between devices in bfloat16 or wider.
A program may use at most 1 GiB of HBM per device.

```python
import jax
import jax.numpy as jnp
from jax import lax

GROUP_SIZE = 4
BATCH_DEV = 128
SEQ_LEN = 512
D_MODEL = 256
NUM_HEADS = 2
EXPERTS = 64
TOP_K = 6
FF_EXPERT = 176
FF_SHARED = 352
CAPACITY = 24
LAYERS = 2
LATENT = 512
ROPE_DIM = 64

KV_DIM = LATENT + ROPE_DIM
TOKENS = GROUP_SIZE * BATCH_DEV
BUFFER_ROWS = EXPERTS * GROUP_SIZE * CAPACITY
ATT_SCALE = 1.0 / (192.0 ** 0.5)
NORM_EPS = 1e-6


def scaled_normal(key, shape, scale):
    return (jax.random.normal(key, shape, jnp.float32) * scale).astype(jnp.bfloat16)


def draw_routing(key):
    key_bias, key_score, key_hot = jax.random.split(key, 3)
    expert_bias = jax.random.randint(key_bias, (LAYERS, 1, EXPERTS), 0, 512)
    raw_score = jax.random.randint(key_score, (LAYERS, TOKENS, EXPERTS), 0, 1024) + expert_bias
    hot_expert = jax.random.randint(key_hot, (LAYERS, GROUP_SIZE, 1, 1), 0, EXPERTS)
    first_rows = jnp.arange(BATCH_DEV)[None, None, :, None] < CAPACITY
    forced = jnp.logical_and(first_rows, jnp.arange(EXPERTS)[None, None, None, :] == hot_expert)
    raw_score = raw_score + 4096 * forced.astype(jnp.int32).reshape(LAYERS, TOKENS, EXPERTS)
    ranked = raw_score * EXPERTS + jnp.arange(EXPERTS)
    expert_ids = lax.top_k(ranked, TOP_K)[1].astype(jnp.int32)
    member = (expert_ids[:, :, :, None] == jnp.arange(EXPERTS)).astype(jnp.int32)
    member = member.reshape(LAYERS, GROUP_SIZE, BATCH_DEV * TOP_K, EXPERTS)
    slot_rank = jnp.sum(jnp.cumsum(member, axis=2) * member, axis=-1) - 1
    slot_rank = slot_rank.reshape(LAYERS, TOKENS, TOP_K)
    slots = jnp.where(slot_rank < CAPACITY, slot_rank, -1).astype(jnp.int32)
    return expert_ids, slots


def setup_inputs(seed: int = 0, part: int = 0) -> dict:
    part_keys = jax.random.split(jax.random.fold_in(jax.random.key(seed), part), 5)
    weight_keys = jax.random.split(jax.random.key(seed + 1), 8)
    x = scaled_normal(part_keys[0], (TOKENS, D_MODEL), 1.0)
    lengths = jax.random.randint(part_keys[1], (TOKENS,), 1, SEQ_LEN + 1).at[0].set(SEQ_LEN).astype(jnp.int32)
    cache = scaled_normal(part_keys[2], (LAYERS, TOKENS, SEQ_LEN, KV_DIM), 1.0)
    expert_ids, slots = draw_routing(part_keys[3])
    route_w = jax.random.uniform(part_keys[4], (LAYERS, TOKENS, TOP_K), jnp.float32, 0.5, 1.5) * (3.0 / TOP_K)
    return dict(
        x=x,
        lengths=lengths,
        cache=cache,
        w_q=scaled_normal(weight_keys[0], (LAYERS, D_MODEL, NUM_HEADS * KV_DIM), 1.5 * D_MODEL ** -0.5),
        w_o=scaled_normal(weight_keys[1], (LAYERS, NUM_HEADS * LATENT, D_MODEL), (NUM_HEADS * LATENT) ** -0.5),
        expert_ids=expert_ids,
        slots=slots,
        route_w=route_w,
        w1_exp=scaled_normal(weight_keys[2], (LAYERS, EXPERTS, D_MODEL, FF_EXPERT), D_MODEL ** -0.5),
        w3_exp=scaled_normal(weight_keys[3], (LAYERS, EXPERTS, D_MODEL, FF_EXPERT), D_MODEL ** -0.5),
        w2_exp=scaled_normal(weight_keys[4], (LAYERS, EXPERTS, FF_EXPERT, D_MODEL), 1.5 * FF_EXPERT ** -0.5),
        w1_sh=scaled_normal(weight_keys[5], (LAYERS, D_MODEL, FF_SHARED), D_MODEL ** -0.5),
        w3_sh=scaled_normal(weight_keys[6], (LAYERS, D_MODEL, FF_SHARED), D_MODEL ** -0.5),
        w2_sh=scaled_normal(weight_keys[7], (LAYERS, FF_SHARED, D_MODEL), 2.0 * FF_SHARED ** -0.5),
    )


def rms_norm(values):
    vals32 = values.astype(jnp.float32)
    return vals32 * lax.rsqrt(jnp.mean(vals32 * vals32, axis=-1, keepdims=True) + NORM_EPS)


def attend_block(block_args):
    q_block, cache_block, len_block = block_args
    scores = jnp.einsum('bhc,btc->bht', q_block.astype(jnp.float32), cache_block.astype(jnp.float32)) * ATT_SCALE
    valid = jnp.arange(SEQ_LEN)[None, None, :] < len_block[:, None, None]
    probs = jax.nn.softmax(jnp.where(valid, scores, -jnp.inf), axis=-1)
    probs = probs.astype(jnp.bfloat16).astype(jnp.float32)
    return jnp.einsum('bht,btc->bhc', probs, cache_block[:, :, :LATENT].astype(jnp.float32))


def reference(x, lengths, cache, w_q, w_o, expert_ids, slots, route_w, w1_exp, w3_exp, w2_exp, w1_sh, w3_sh, w2_sh):
    owner_dev = jnp.arange(TOKENS) // BATCH_DEV
    len_blocks = lengths.reshape(GROUP_SIZE, BATCH_DEV)

    def layer_step(resid, layer_args):
        cache_l, w_q_l, w_o_l, ids_l, slot_l, gate_w, w1_e, w3_e, w2_e, w1_s, w3_s, w2_s = layer_args
        normed = rms_norm(resid).astype(jnp.bfloat16)
        queries = jnp.dot(normed, w_q_l, preferred_element_type=jnp.float32).astype(jnp.bfloat16)
        queries = queries.reshape(GROUP_SIZE, BATCH_DEV, NUM_HEADS, KV_DIM)
        attn = lax.map(attend_block, (queries, cache_l.reshape(GROUP_SIZE, BATCH_DEV, SEQ_LEN, KV_DIM), len_blocks))
        attn = attn.astype(jnp.bfloat16).reshape(TOKENS, NUM_HEADS * LATENT)
        resid = (resid.astype(jnp.float32) + jnp.dot(attn, w_o_l, preferred_element_type=jnp.float32)).astype(jnp.bfloat16)
        ffn_in = rms_norm(resid).astype(jnp.bfloat16)
        shared_gate = jnp.dot(ffn_in, w3_s, preferred_element_type=jnp.float32)
        shared_up = jnp.dot(ffn_in, w1_s, preferred_element_type=jnp.float32)
        shared_h = (jax.nn.silu(shared_gate) * shared_up).astype(jnp.bfloat16)
        shared_out = jnp.dot(shared_h, w2_s, preferred_element_type=jnp.float32)
        buf_rows = jnp.where(slot_l >= 0, ids_l * (GROUP_SIZE * CAPACITY) + owner_dev[:, None] * CAPACITY + slot_l, BUFFER_ROWS)
        copies = jnp.broadcast_to(ffn_in[:, None, :], (TOKENS, TOP_K, D_MODEL)).reshape(TOKENS * TOP_K, D_MODEL)
        buffer = jnp.zeros((BUFFER_ROWS, D_MODEL), jnp.bfloat16).at[buf_rows.reshape(-1)].set(copies, mode='drop')
        buffer = buffer.reshape(EXPERTS, GROUP_SIZE * CAPACITY, D_MODEL).astype(jnp.float32)
        gate_in = jnp.einsum('ecd,edf->ecf', buffer, w3_e.astype(jnp.float32))
        up_in = jnp.einsum('ecd,edf->ecf', buffer, w1_e.astype(jnp.float32))
        hidden = (jax.nn.silu(gate_in) * up_in).astype(jnp.bfloat16).astype(jnp.float32)
        expert_out = jnp.einsum('ecf,efd->ecd', hidden, w2_e.astype(jnp.float32)).astype(jnp.bfloat16)
        picked = jnp.take(expert_out.reshape(BUFFER_ROWS, D_MODEL), buf_rows, axis=0, mode='fill', fill_value=0)
        routed = jnp.sum(gate_w[:, :, None] * picked.astype(jnp.float32), axis=1)
        resid = (resid.astype(jnp.float32) + routed + shared_out).astype(jnp.bfloat16)
        return resid, None

    final_x = lax.scan(layer_step, x, (cache, w_q, w_o, expert_ids, slots, route_w, w1_exp, w3_exp, w2_exp, w1_sh, w3_sh, w2_sh))[0]
    return final_x
```

```python
import functools
import jax
import jax.numpy as jnp
from jax import lax
from jax.experimental import pallas as pl
from jax.experimental.pallas import tpu as pltpu
from jax.sharding import PartitionSpec as P

NORM_EPS = 1e-6
ATT_SCALE = 1.0 / (192.0 ** 0.5)
LATENT = 512
CHUNK = 128
F32 = jnp.float32
BF16 = jnp.bfloat16


def rms_norm(values):
    vals32 = values.astype(F32)
    return vals32 * lax.rsqrt(jnp.mean(vals32 * vals32, axis=-1, keepdims=True) + NORM_EPS)


def bucket_order(lengths):
    count = lengths.shape[0]
    chunks = (lengths + (CHUNK - 1)) // CHUNK
    ids = jnp.arange(count, dtype=jnp.int32)
    ahead = (chunks[None, :] > chunks[:, None]) | ((chunks[None, :] == chunks[:, None]) & (ids[None, :] < ids[:, None]))
    place = jnp.sum(ahead.astype(jnp.int32), axis=1)
    hit = place[None, :] == ids[:, None]
    order = jnp.sum(jnp.where(hit, ids[None, :], 0), axis=1)
    sorted_len = jnp.sum(jnp.where(hit, lengths[None, :], 0), axis=1)
    return place, order, sorted_len


def attn_kernel(layer, slots, order_ref, slen_ref, place_ref, x_ref, cache_ref, wq_hbm, wo_hbm,
                x_out, g_out, wq, wo, buf, qbd, obuf, pbuf, sem, wsem):
    toks, d_model = x_ref.shape
    kv_dim, seq_len = cache_ref.shape[2], cache_ref.shape[3]
    rope = kv_dim - LATENT
    groups = toks // 8
    max_n = seq_len // CHUNK

    def group_n(g):
        return lax.div(slen_ref[g * 8] + (CHUNK - 1), CHUNK)

    def start_group(g):
        slot = lax.rem(g, slots)
        n = group_n(g)
        for nn in range(1, max_n + 1):
            @pl.when(n == nn)
            def _():
                for i in range(8):
                    b = order_ref[g * 8 + i]
                    half, j = i // 4, i % 4
                    cols = pl.ds(0, nn * CHUNK)
                    pltpu.make_async_copy(
                        cache_ref.at[layer, b, pl.ds(0, LATENT), cols],
                        buf.at[slot, half, pl.ds(j * LATENT, LATENT), cols], sem.at[slot]).start()
                    pltpu.make_async_copy(
                        cache_ref.at[layer, b, pl.ds(LATENT, rope), cols],
                        buf.at[slot, half, pl.ds(4 * LATENT + j * rope, rope), cols], sem.at[slot]).start()

    wq_copy = pltpu.make_async_copy(wq_hbm.at[layer], wq, wsem.at[0])
    wo_copy = pltpu.make_async_copy(wo_hbm.at[layer], wo, wsem.at[1])
    wq_copy.start()
    for g in range(slots):
        start_group(g)
    wo_copy.start()

    rows = 2 * toks
    row_id = lax.broadcasted_iota(jnp.int32, (rows, toks), 0)
    place = place_ref[...]
    base = lax.shift_right_logical(place, 2) * 8 + lax.rem(place, 4)
    pick0 = (row_id == base).astype(BF16)
    pick1 = (row_id == base + 4).astype(BF16)
    h = rms_norm(x_ref[...]).astype(BF16)
    wq_copy.wait()
    q = jnp.dot(h, wq[...], preferred_element_type=F32).astype(BF16)
    qrows = (jnp.dot(pick0, q[:, :kv_dim], preferred_element_type=F32)
             + jnp.dot(pick1, q[:, kv_dim:], preferred_element_type=F32))
    sub = lax.rem(lax.broadcasted_iota(jnp.int32, (rows, 1), 0), 4)
    for j in range(4):
        qbd[:, j * LATENT:(j + 1) * LATENT] = jnp.where(sub == j, qrows[:, :LATENT], 0.0).astype(BF16)
    tail = qrows[:, LATENT:]
    tail2 = jnp.concatenate([tail, tail], axis=1)
    lane = lax.broadcasted_iota(jnp.int32, (rows, 2 * rope), 1)
    for jj in range(2):
        keep = sub == (2 * jj + (lane >= rope).astype(jnp.int32))
        qbd[:, 4 * LATENT + jj * 2 * rope:4 * LATENT + (jj + 1) * 2 * rope] = jnp.where(keep, tail2, 0.0).astype(BF16)

    row16 = lax.broadcasted_iota(jnp.int32, (16, CHUNK), 0)
    sub16 = lax.rem(row16, 4)
    lane16 = lax.broadcasted_iota(jnp.int32, (16, CHUNK), 1)
    half16 = (row16 >= 8).astype(jnp.int32)
    seq16 = half16 * 4 + sub16

    def scores(g, nn):
        slot = lax.rem(g, slots)
        lhs = qbd[pl.ds(pl.multiple_of(g * 16, 16), 16), :]
        lens = jnp.zeros((16, CHUNK), jnp.int32)
        for i in range(8):
            lens = jnp.where(seq16 == i, slen_ref[g * 8 + i], lens)
        out = []
        for k in range(nn):
            cols = pl.ds(k * CHUNK, CHUNK)
            rhs = jnp.concatenate([buf[slot, 0, :, cols], buf[slot, 1, :, cols]], axis=1)
            raw = jnp.dot(lhs, rhs, preferred_element_type=F32)
            s = jnp.concatenate([raw[0:8, :CHUNK], raw[8:16, CHUNK:]], axis=0) * ATT_SCALE
            out.append(jnp.where(lane16 + k * CHUNK < lens, s, -jnp.inf))
        return out

    def softmax(s):
        m = s[0]
        for t in s[1:]:
            m = jnp.maximum(m, t)
        m = jnp.max(m, axis=1, keepdims=True)
        e = [jnp.exp(t - m) for t in s]
        tot = e[0]
        for t in e[1:]:
            tot = tot + t
        inv = 1.0 / jnp.sum(tot, axis=1, keepdims=True)
        return [(t * inv) for t in e]

    def values(g, p):
        slot = lax.rem(g, slots)
        lhs, rhs = [], []
        for k, t in enumerate(p):
            cols = pl.ds(k * CHUNK, CHUNK)
            for j in range(4):
                for half in range(2):
                    keep = (sub16 == j) & (half16 == half)
                    lhs.append(jnp.where(keep, t, 0.0).astype(BF16))
                    rhs.append(buf[slot, half, pl.ds(j * LATENT, LATENT), cols])
        o = lax.dot_general(jnp.concatenate(lhs, axis=1), jnp.concatenate(rhs, axis=1),
                            (((1,), (1,)), ((), ())), preferred_element_type=F32)
        obuf[pl.ds(pl.multiple_of(g * 16, 16), 16), :] = o.astype(BF16)

    def wait_group(g, nn):
        slot = lax.rem(g, slots)
        view = buf.at[slot, :, :, pl.ds(0, nn * CHUNK)]
        pltpu.make_async_copy(view, view, sem.at[slot]).wait()

    def stage_scores(g, nn):
        p = softmax(scores(g, nn))
        for k, t in enumerate(p):
            pbuf[lax.rem(g, 2), k] = t

    def stage_values(g, nn):
        values(g, [pbuf[lax.rem(g, 2), k] for k in range(nn)])

    def each_n(n, fn):
        for nn in range(1, max_n + 1):
            pl.when(n == nn)(functools.partial(fn, nn))

    def first(nn):
        wait_group(0, nn)
        stage_scores(0, nn)
    each_n(group_n(0), first)

    def body(g, _):
        n_prev = group_n(g - 1)
        n_cur = group_n(g)

        @pl.when(n_prev == n_cur)
        def _():
            def both(nn):
                wait_group(g, nn)
                p_prev = [pbuf[lax.rem(g - 1, 2), k] for k in range(nn)]
                s = scores(g, nn)
                values(g - 1, p_prev)
                for k, t in enumerate(softmax(s)):
                    pbuf[lax.rem(g, 2), k] = t
            each_n(n_cur, both)

        @pl.when(n_prev != n_cur)
        def _():
            each_n(n_prev, functools.partial(stage_values, g - 1))
            def only(nn):
                wait_group(g, nn)
                stage_scores(g, nn)
            each_n(n_cur, only)

        @pl.when(g - 1 + slots < groups)
        def _():
            start_group(g - 1 + slots)
        return 0

    lax.fori_loop(1, groups, body, 0)
    each_n(group_n(groups - 1), functools.partial(stage_values, groups - 1))

    wo_copy.wait()
    picked = obuf[...]
    total = x_ref[...].astype(F32)
    for head, pick in enumerate((pick0, pick1)):
        o = lax.dot_general(pick, picked, (((0,), (0,)), ((), ())), preferred_element_type=F32).astype(BF16)
        total = total + jnp.dot(o, wo[head * LATENT:(head + 1) * LATENT, :], preferred_element_type=F32)
    x_new = total.astype(BF16)
    x_out[...] = x_new
    g_out[...] = rms_norm(x_new).astype(BF16)


def attention(layer, place, order, sorted_len, x, cache_t, w_q, w_o, slots=8):
    toks, d_model = x.shape
    kv_dim, seq_len = cache_t.shape[2], cache_t.shape[3]
    any_spec = pl.BlockSpec(memory_space=pl.ANY)
    smem = pl.BlockSpec(memory_space=pltpu.SMEM)
    vmem = pl.BlockSpec(memory_space=pltpu.VMEM)
    return pl.pallas_call(
        functools.partial(attn_kernel, layer, slots),
        out_shape=(jax.ShapeDtypeStruct((toks, d_model), BF16), jax.ShapeDtypeStruct((toks, d_model), BF16)),
        in_specs=[smem, smem, vmem, vmem, any_spec, any_spec, any_spec],
        out_specs=(vmem, vmem),
        scratch_shapes=[
            pltpu.VMEM(w_q.shape[1:], BF16),
            pltpu.VMEM(w_o.shape[1:], BF16),
            pltpu.VMEM((slots, 2, 4 * kv_dim, seq_len), BF16),
            pltpu.VMEM((2 * toks, 4 * kv_dim), BF16),
            pltpu.VMEM((2 * toks, LATENT), BF16),
            pltpu.VMEM((2, seq_len // CHUNK, 16, CHUNK), F32),
            pltpu.SemaphoreType.DMA((slots,)),
            pltpu.SemaphoreType.DMA((2,)),
        ],
        compiler_params=pltpu.CompilerParams(vmem_limit_bytes=48 * 1024 * 1024),
        name="latent_attention",
    )(order, sorted_len, place.reshape(1, toks), x, cache_t, w_q, w_o)


def gated_hidden(tok_in, w_up, w_gate):
    gate_in = jnp.dot(tok_in, w_gate, preferred_element_type=jnp.float32)
    up_in = jnp.dot(tok_in, w_up, preferred_element_type=jnp.float32)
    return (jax.nn.silu(gate_in) * up_in).astype(jnp.bfloat16)


def route_select(ids_l, slot_l, experts, capacity):
    buf_rows = jnp.where(slot_l >= 0, ids_l * capacity + slot_l, -1)
    return (buf_rows[:, :, None] == jnp.arange(experts * capacity)).astype(jnp.bfloat16)


def solution(mesh):
    group = mesh.shape['dp']
    tok_axes = ('replica', 'dp')
    in_specs = (
        P(tok_axes, None), P(tok_axes), P(None, tok_axes, None, None),
        P(None, None, None), P(None, None, None),
        P(None, tok_axes, None), P(None, tok_axes, None), P(None, tok_axes, None),
        P(None, 'dp', None, None), P(None, 'dp', None, None), P(None, 'dp', None, None),
        P(None, None, 'dp'), P(None, None, 'dp'), P(None, 'dp', None),
    )

    def device_step(x, lengths, cache, w_q, w_o, expert_ids, slots, route_w, w1_exp, w3_exp, w2_exp, w1_sh, w3_sh, w2_sh):
        batch_dev, d_model = x.shape
        local_experts = w1_exp.shape[1]
        experts = local_experts * group
        top_k = expert_ids.shape[2]
        capacity = max(1, (2 * batch_dev * top_k) // experts)
        resid = x
        place, order, sorted_len = bucket_order(lengths)
        cache_t = jnp.swapaxes(cache, 2, 3)
        for layer_idx in range(cache.shape[0]):
            resid, ffn_in = attention(layer_idx, place, order, sorted_len, resid, cache_t, w_q, w_o)
            gathered = lax.all_gather(ffn_in, 'dp', axis=0, tiled=True)
            shared_h = gated_hidden(gathered, w1_sh[layer_idx], w3_sh[layer_idx])
            shared_part = jnp.dot(shared_h, w2_sh[layer_idx], preferred_element_type=jnp.float32)
            shared_out = lax.psum_scatter(shared_part, 'dp', scatter_dimension=0, tiled=True)
            select = route_select(expert_ids[layer_idx], slots[layer_idx], experts, capacity)
            dispatch = jnp.sum(select, axis=1)
            send_buf = jnp.einsum('br,bd->rd', dispatch, ffn_in, preferred_element_type=jnp.float32).astype(jnp.bfloat16)
            send_buf = send_buf.reshape(group, local_experts, capacity, d_model)
            recv_buf = lax.all_to_all(send_buf, 'dp', 0, 0, tiled=True)
            gate_in = jnp.einsum('sncd,ndf->nscf', recv_buf, w3_exp[layer_idx], preferred_element_type=jnp.float32)
            up_in = jnp.einsum('sncd,ndf->nscf', recv_buf, w1_exp[layer_idx], preferred_element_type=jnp.float32)
            hidden = (jax.nn.silu(gate_in) * up_in).astype(jnp.bfloat16)
            expert_out = jnp.einsum('nscf,nfd->sncd', hidden, w2_exp[layer_idx], preferred_element_type=jnp.float32).astype(jnp.bfloat16)
            returned = lax.all_to_all(expert_out, 'dp', 0, 0, tiled=True)
            returned = returned.reshape(experts * capacity, d_model)
            picked = jnp.einsum('cls,se->cle', select, returned, preferred_element_type=jnp.float32)
            routed = jnp.sum(route_w[layer_idx][:, :, None] * picked, axis=1)
            resid = (resid.astype(jnp.float32) + routed + shared_out).astype(jnp.bfloat16)
        return resid

    return jax.shard_map(device_step, mesh=mesh, in_specs=in_specs, out_specs=P(tok_axes, None), check_vma=False)
```

```python
import functools
import jax
import jax.numpy as jnp
from jax import lax
from jax.experimental import pallas as pl
from jax.experimental.pallas import tpu as pltpu
from jax.sharding import PartitionSpec as P

NORM_EPS = 1e-6
ATT_SCALE = 1.0 / (192.0 ** 0.5)
LATENT = 512
CHUNK = 128
F32 = jnp.float32
BF16 = jnp.bfloat16


def rms_norm(values):
    vals32 = values.astype(F32)
    return vals32 * lax.rsqrt(jnp.mean(vals32 * vals32, axis=-1, keepdims=True) + NORM_EPS)


def bucket_order(lengths):
    count = lengths.shape[0]
    chunks = (lengths + (CHUNK - 1)) // CHUNK
    ids = jnp.arange(count, dtype=jnp.int32)
    ahead = (chunks[None, :] > chunks[:, None]) | ((chunks[None, :] == chunks[:, None]) & (ids[None, :] < ids[:, None]))
    place = jnp.sum(ahead.astype(jnp.int32), axis=1)
    hit = place[None, :] == ids[:, None]
    order = jnp.sum(jnp.where(hit, ids[None, :], 0), axis=1)
    sorted_len = jnp.sum(jnp.where(hit, lengths[None, :], 0), axis=1)
    return place, order, sorted_len


def attn_kernel(layer, slots, order_ref, slen_ref, place_ref, x_ref, cache_ref, wq_hbm, wo_hbm,
                ids_ref, slot_ref, route_ref, x_out, g_out, wt_out, wq, wo, buf, qbd, obuf, pbuf, sem, wsem):
    toks, d_model = x_ref.shape
    kv_dim, seq_len = cache_ref.shape[2], cache_ref.shape[3]
    rope = kv_dim - LATENT
    groups = toks // 8
    max_n = seq_len // CHUNK

    def group_n(g):
        return lax.div(slen_ref[g * 8] + (CHUNK - 1), CHUNK)

    def start_group(g):
        slot = lax.rem(g, slots)
        n = group_n(g)
        for nn in range(1, max_n + 1):
            @pl.when(n == nn)
            def _():
                for i in range(8):
                    b = order_ref[g * 8 + i]
                    half, j = i // 4, i % 4
                    cols = pl.ds(0, nn * CHUNK)
                    pltpu.make_async_copy(
                        cache_ref.at[layer, b, pl.ds(0, LATENT), cols],
                        buf.at[slot, half, pl.ds(j * LATENT, LATENT), cols], sem.at[slot]).start()
                    pltpu.make_async_copy(
                        cache_ref.at[layer, b, pl.ds(LATENT, rope), cols],
                        buf.at[slot, half, pl.ds(4 * LATENT + j * rope, rope), cols], sem.at[slot]).start()

    wq_copy = pltpu.make_async_copy(wq_hbm.at[layer], wq, wsem.at[0])
    wo_copy = pltpu.make_async_copy(wo_hbm.at[layer], wo, wsem.at[1])
    wq_copy.start()
    for g in range(slots):
        start_group(g)
    wo_copy.start()

    experts = wt_out.shape[0]
    expert_id = lax.broadcasted_iota(jnp.int32, (experts, toks), 0)
    wt = jnp.zeros((experts, toks), F32)
    for j in range(ids_ref.shape[0]):
        at = pl.ds(layer, 1)
        hit = (ids_ref[j, at, :] == expert_id) & (slot_ref[j, at, :] >= 0)
        wt = wt + jnp.where(hit, route_ref[j, at, :], 0.0)
    wt_out[...] = wt

    rows = 2 * toks
    row_id = lax.broadcasted_iota(jnp.int32, (rows, toks), 0)
    place = place_ref[...]
    base = lax.shift_right_logical(place, 2) * 8 + lax.rem(place, 4)
    pick0 = (row_id == base).astype(BF16)
    pick1 = (row_id == base + 4).astype(BF16)
    h = rms_norm(x_ref[...]).astype(BF16)
    wq_copy.wait()
    q = jnp.dot(h, wq[...], preferred_element_type=F32).astype(BF16)
    qrows = (jnp.dot(pick0, q[:, :kv_dim], preferred_element_type=F32)
             + jnp.dot(pick1, q[:, kv_dim:], preferred_element_type=F32))
    sub = lax.rem(lax.broadcasted_iota(jnp.int32, (rows, 1), 0), 4)
    for j in range(4):
        qbd[:, j * LATENT:(j + 1) * LATENT] = jnp.where(sub == j, qrows[:, :LATENT], 0.0).astype(BF16)
    tail = qrows[:, LATENT:]
    tail2 = jnp.concatenate([tail, tail], axis=1)
    lane = lax.broadcasted_iota(jnp.int32, (rows, 2 * rope), 1)
    for jj in range(2):
        keep = sub == (2 * jj + (lane >= rope).astype(jnp.int32))
        qbd[:, 4 * LATENT + jj * 2 * rope:4 * LATENT + (jj + 1) * 2 * rope] = jnp.where(keep, tail2, 0.0).astype(BF16)

    row16 = lax.broadcasted_iota(jnp.int32, (16, CHUNK), 0)
    sub16 = lax.rem(row16, 4)
    lane16 = lax.broadcasted_iota(jnp.int32, (16, CHUNK), 1)
    half16 = (row16 >= 8).astype(jnp.int32)
    seq16 = half16 * 4 + sub16

    def scores(g, nn):
        slot = lax.rem(g, slots)
        lhs = qbd[pl.ds(pl.multiple_of(g * 16, 16), 16), :]
        lens = jnp.zeros((16, CHUNK), jnp.int32)
        for i in range(8):
            lens = jnp.where(seq16 == i, slen_ref[g * 8 + i], lens)
        out = []
        for k in range(nn):
            cols = pl.ds(k * CHUNK, CHUNK)
            rhs = jnp.concatenate([buf[slot, 0, :, cols], buf[slot, 1, :, cols]], axis=1)
            raw = jnp.dot(lhs, rhs, preferred_element_type=F32)
            s = jnp.concatenate([raw[0:8, :CHUNK], raw[8:16, CHUNK:]], axis=0) * ATT_SCALE
            out.append(jnp.where(lane16 + k * CHUNK < lens, s, -jnp.inf))
        return out

    def softmax(s):
        m = s[0]
        for t in s[1:]:
            m = jnp.maximum(m, t)
        m = jnp.max(m, axis=1, keepdims=True)
        e = [jnp.exp(t - m) for t in s]
        tot = e[0]
        for t in e[1:]:
            tot = tot + t
        inv = 1.0 / jnp.sum(tot, axis=1, keepdims=True)
        return [(t * inv) for t in e]

    def values(g, p):
        slot = lax.rem(g, slots)
        lhs, rhs = [], []
        for k, t in enumerate(p):
            cols = pl.ds(k * CHUNK, CHUNK)
            for j in range(4):
                for half in range(2):
                    keep = (sub16 == j) & (half16 == half)
                    lhs.append(jnp.where(keep, t, 0.0).astype(BF16))
                    rhs.append(buf[slot, half, pl.ds(j * LATENT, LATENT), cols])
        o = lax.dot_general(jnp.concatenate(lhs, axis=1), jnp.concatenate(rhs, axis=1),
                            (((1,), (1,)), ((), ())), preferred_element_type=F32)
        obuf[pl.ds(pl.multiple_of(g * 16, 16), 16), :] = o.astype(BF16)

    def wait_group(g, nn):
        slot = lax.rem(g, slots)
        view = buf.at[slot, :, :, pl.ds(0, nn * CHUNK)]
        pltpu.make_async_copy(view, view, sem.at[slot]).wait()

    def stage_scores(g, nn):
        p = softmax(scores(g, nn))
        for k, t in enumerate(p):
            pbuf[lax.rem(g, 2), k] = t

    def stage_values(g, nn):
        values(g, [pbuf[lax.rem(g, 2), k] for k in range(nn)])

    def each_n(n, fn):
        for nn in range(1, max_n + 1):
            pl.when(n == nn)(functools.partial(fn, nn))

    def first(nn):
        wait_group(0, nn)
        stage_scores(0, nn)
    each_n(group_n(0), first)

    def body(g, _):
        n_prev = group_n(g - 1)
        n_cur = group_n(g)

        @pl.when(n_prev == n_cur)
        def _():
            def both(nn):
                wait_group(g, nn)
                p_prev = [pbuf[lax.rem(g - 1, 2), k] for k in range(nn)]
                s = scores(g, nn)
                values(g - 1, p_prev)
                for k, t in enumerate(softmax(s)):
                    pbuf[lax.rem(g, 2), k] = t
            each_n(n_cur, both)

        @pl.when(n_prev != n_cur)
        def _():
            each_n(n_prev, functools.partial(stage_values, g - 1))
            def only(nn):
                wait_group(g, nn)
                stage_scores(g, nn)
            each_n(n_cur, only)

        @pl.when(g - 1 + slots < groups)
        def _():
            start_group(g - 1 + slots)
        return 0

    lax.fori_loop(1, groups, body, 0)
    each_n(group_n(groups - 1), functools.partial(stage_values, groups - 1))

    wo_copy.wait()
    picked = obuf[...]
    total = x_ref[...].astype(F32)
    for head, pick in enumerate((pick0, pick1)):
        o = lax.dot_general(pick, picked, (((0,), (0,)), ((), ())), preferred_element_type=F32).astype(BF16)
        total = total + jnp.dot(o, wo[head * LATENT:(head + 1) * LATENT, :], preferred_element_type=F32)
    x_new = total.astype(BF16)
    x_out[...] = x_new
    g_out[...] = rms_norm(x_new).astype(BF16)


def attention(layer, place, order, sorted_len, x, cache_t, w_q, w_o, ids, slot, route_w, experts, slots=8):
    toks, d_model = x.shape
    kv_dim, seq_len = cache_t.shape[2], cache_t.shape[3]
    any_spec = pl.BlockSpec(memory_space=pl.ANY)
    smem = pl.BlockSpec(memory_space=pltpu.SMEM)
    vmem = pl.BlockSpec(memory_space=pltpu.VMEM)
    return pl.pallas_call(
        functools.partial(attn_kernel, layer, slots),
        out_shape=(jax.ShapeDtypeStruct((toks, d_model), BF16), jax.ShapeDtypeStruct((toks, d_model), BF16),
                   jax.ShapeDtypeStruct((experts, toks), F32)),
        in_specs=[smem, smem, vmem, vmem, any_spec, any_spec, any_spec, vmem, vmem, vmem],
        out_specs=(vmem, vmem, vmem),
        scratch_shapes=[
            pltpu.VMEM(w_q.shape[1:], BF16),
            pltpu.VMEM(w_o.shape[1:], BF16),
            pltpu.VMEM((slots, 2, 4 * kv_dim, seq_len), BF16),
            pltpu.VMEM((2 * toks, 4 * kv_dim), BF16),
            pltpu.VMEM((2 * toks, LATENT), BF16),
            pltpu.VMEM((2, seq_len // CHUNK, 16, CHUNK), F32),
            pltpu.SemaphoreType.DMA((slots,)),
            pltpu.SemaphoreType.DMA((2,)),
        ],
        compiler_params=pltpu.CompilerParams(vmem_limit_bytes=48 * 1024 * 1024),
        name="latent_attention",
    )(order, sorted_len, place.reshape(1, toks), x, cache_t, w_q, w_o, ids, slot, route_w)


MESH_ID = pl.DeviceIdType.MESH
EXP_STEP = 4


def moe_kernel(layer, x_ref, g_ref, route_ref, w1_hbm, w3_hbm, w2_hbm, w1s_hbm, w3s_hbm, w2s_hbm, out_ref,
               gall, wall, w1, w3, w2, w2t, w1s, w3s, w2s, acc, part, wsem, gsend, grecv, rsend, rrecv, psend, precv):
    me = lax.axis_index('dp')
    core = lax.rem(me, 2)
    chip = lax.div(me, 2)
    partner = chip * 2 + (1 - core)
    cross = (1 - chip) * 2 + (1 - core)
    same = (1 - chip) * 2 + core
    peers = (partner, cross, same)
    experts, ff, d_model = w2.shape
    toks = x_ref.shape[0]

    loads = [pltpu.make_async_copy(src.at[layer], dst, wsem.at[i]) for i, (src, dst) in enumerate(
        ((w2_hbm, w2), (w1_hbm, w1), (w3_hbm, w3), (w1s_hbm, w1s), (w3s_hbm, w3s), (w2s_hbm, w2s)))]
    for c in loads:
        c.start()

    barrier = pltpu.get_barrier_semaphore()
    for p in peers:
        pl.semaphore_signal(barrier, inc=1, device_id={'dp': p}, device_id_type=MESH_ID)
    pl.semaphore_wait(barrier, 3)

    gcopies, rcopies = [], []
    for i, p in enumerate(peers):
        rcopies.append(pltpu.make_async_remote_copy(
            route_ref.at[pl.ds(p * experts, experts)], wall.at[i + 1], rsend.at[i], rrecv.at[i],
            device_id={'dp': p}, device_id_type=MESH_ID))
        gcopies.append(pltpu.make_async_remote_copy(
            g_ref, gall.at[i + 1], gsend.at[i], grecv.at[i], device_id={'dp': p}, device_id_type=MESH_ID))
    for i in range(3):
        rcopies[i].start()
        gcopies[i].start()

    gall[0] = g_ref[...]
    wall[0] = route_ref[pl.ds(pl.multiple_of(me * experts, experts), experts), :]
    for c in loads:
        c.wait()

    def flip(e, carry):
        w2t[e] = w2[e].T
        return carry
    lax.fori_loop(0, experts, flip, 0)
    w2st = w2s[...].T

    def gated(w3_rows, w1_rows, tok):
        dims = (((1,), (1,)), ((), ()))
        gate = lax.dot_general(w3_rows, tok, dims, preferred_element_type=F32)
        up = lax.dot_general(w1_rows, tok, dims, preferred_element_type=F32)
        return (gate * (1.0 / (1.0 + jnp.exp(-gate))) * up).astype(BF16)

    def ffn(pair):
        tok = jnp.concatenate([gall[2 * pair], gall[2 * pair + 1]], axis=0)
        acc[pair] = jnp.dot(w2st, gated(w3s[...], w1s[...], tok), preferred_element_type=F32)

        def step(s, carry):
            rows = pl.ds(pl.multiple_of(s * (EXP_STEP * ff), 16), EXP_STEP * ff)
            hid = gated(w3[rows, :], w1[rows, :], tok)
            total = acc[pair]
            for i in range(EXP_STEP):
                e = s * EXP_STEP + i
                u = jnp.dot(w2t[e], hid[i * ff:(i + 1) * ff], preferred_element_type=F32)
                u = u.astype(BF16).astype(F32)
                w = jnp.concatenate([wall[2 * pair, pl.ds(e, 1), :], wall[2 * pair + 1, pl.ds(e, 1), :]], axis=1)
                total = total + jnp.where(w > 0.0, u * w, 0.0)
            acc[pair] = total
            return carry
        lax.fori_loop(0, experts // EXP_STEP, step, 0)

    def send_part(i, src, dst):
        return pltpu.make_async_remote_copy(
            src, part.at[i], psend.at[i], precv.at[i], device_id={'dp': dst}, device_id_type=MESH_ID)

    rcopies[0].wait_recv()
    gcopies[0].wait_recv()
    ffn(0)
    stage = acc.at[2, :, pl.ds(0, toks)]
    home = send_part(0, acc.at[0, :, pl.ds(toks, toks)], partner)
    home.start()

    for i in (1, 2):
        rcopies[i].wait_recv()
        gcopies[i].wait_recv()
    ffn(1)
    relay = send_part(1, acc.at[1, :, pl.ds(0, toks)], partner)
    relay.start()
    relay.wait_recv()
    acc[2, :, :toks] = acc[1, :, toks:] + part[1]
    far = send_part(2, stage, same)
    far.start()
    home.wait_recv()
    near = acc[0, :, :toks] + part[0]
    far.wait_recv()
    out_ref[...] = (x_ref[...].astype(F32) + (near + part[2]).T).astype(BF16)

    for c in gcopies + rcopies + [home, relay, far]:
        c.wait_send()


def moe(layer, x, g, route, w1, w3, w2, w1s, w3s, w2s):
    toks, d_model = x.shape
    _, experts, ff, _ = w2.shape
    shared = w2s.shape[1]
    any_spec = pl.BlockSpec(memory_space=pl.ANY)
    vmem = pl.BlockSpec(memory_space=pltpu.VMEM)
    dma = pltpu.SemaphoreType.DMA
    return pl.pallas_call(
        functools.partial(moe_kernel, layer),
        out_shape=jax.ShapeDtypeStruct((toks, d_model), BF16),
        in_specs=[vmem] * 3 + [any_spec] * 6,
        out_specs=vmem,
        scratch_shapes=[
            pltpu.VMEM((4, toks, d_model), BF16),
            pltpu.VMEM((4, experts, toks), F32),
            pltpu.VMEM((experts * ff, d_model), BF16),
            pltpu.VMEM((experts * ff, d_model), BF16),
            pltpu.VMEM((experts, ff, d_model), BF16),
            pltpu.VMEM((experts, d_model, ff), BF16),
            pltpu.VMEM((shared, d_model), BF16),
            pltpu.VMEM((shared, d_model), BF16),
            pltpu.VMEM((shared, d_model), BF16),
            pltpu.VMEM((3, d_model, 2 * toks), F32),
            pltpu.VMEM((3, d_model, toks), F32),
            dma((6,)), dma((3,)), dma((3,)), dma((3,)), dma((3,)), dma((3,)), dma((3,)),
        ],
        compiler_params=pltpu.CompilerParams(
            collective_id=layer, has_side_effects=True, vmem_limit_bytes=40 * 1024 * 1024),
        name="expert_exchange",
    )(x, g, route, w1, w3, w2, w1s, w3s, w2s)


def solution(mesh):
    tok_axes = ('replica', 'dp')
    in_specs = (
        P(tok_axes, None), P(tok_axes), P(None, tok_axes, None, None),
        P(None, None, None), P(None, None, None),
        P(None, tok_axes, None), P(None, tok_axes, None), P(None, tok_axes, None),
        P(None, 'dp', None, None), P(None, 'dp', None, None), P(None, 'dp', None, None),
        P(None, None, 'dp'), P(None, None, 'dp'), P(None, 'dp', None),
    )

    def device_step(x, lengths, cache, w_q, w_o, expert_ids, slots, route_w, w1_exp, w3_exp, w2_exp, w1_sh, w3_sh, w2_sh):
        layers, local, d_model, ff = w1_exp.shape
        place, order, sorted_len = bucket_order(lengths)
        cache_t = jnp.swapaxes(cache, 2, 3)
        by_choice = [jnp.transpose(a, (2, 0, 1)) for a in (expert_ids, slots, route_w)]
        w1 = jnp.swapaxes(w1_exp, 2, 3).reshape(layers, local * ff, d_model)
        w3 = jnp.swapaxes(w3_exp, 2, 3).reshape(layers, local * ff, d_model)
        w1s, w3s = jnp.swapaxes(w1_sh, 1, 2), jnp.swapaxes(w3_sh, 1, 2)
        experts = local * mesh.shape['dp']
        resid = x
        for layer in range(layers):
            resid, ffn_in, route = attention(layer, place, order, sorted_len, resid, cache_t, w_q, w_o, *by_choice, experts)
            resid = moe(layer, resid, ffn_in, route, w1, w3, w2_exp, w1s, w3s, w2_sh)
        return resid

    return jax.shard_map(device_step, mesh=mesh, in_specs=in_specs, out_specs=P(tok_axes, None), check_vma=False)
```

```python
import functools
import jax
import jax.numpy as jnp
from jax import lax
from jax.experimental import pallas as pl
from jax.experimental.pallas import tpu as pltpu
from jax.sharding import PartitionSpec as P

NORM_EPS = 1e-6
ATT_SCALE = 1.0 / (192.0 ** 0.5)
LATENT = 512
CHUNK = 128
F32 = jnp.float32
BF16 = jnp.bfloat16


def rms_norm(values):
    vals32 = values.astype(F32)
    return vals32 * lax.rsqrt(jnp.mean(vals32 * vals32, axis=-1, keepdims=True) + NORM_EPS)


def bucket_order(lengths):
    count = lengths.shape[0]
    chunks = (lengths + (CHUNK - 1)) // CHUNK
    ids = jnp.arange(count, dtype=jnp.int32)
    ahead = (chunks[None, :] > chunks[:, None]) | ((chunks[None, :] == chunks[:, None]) & (ids[None, :] < ids[:, None]))
    place = jnp.sum(ahead.astype(jnp.int32), axis=1)
    hit = place[None, :] == ids[:, None]
    order = jnp.sum(jnp.where(hit, ids[None, :], 0), axis=1)
    sorted_len = jnp.sum(jnp.where(hit, lengths[None, :], 0), axis=1)
    return place, order, sorted_len


def attn_kernel(layer, slots, order_ref, slen_ref, place_ref, x_in, cache_ref, wq_hbm, wo_hbm,
                x_out, g_out, wq, wo, buf, qbd, obuf, pbuf, sem, wsem, xbuf):
    toks, d_model = x_in.shape
    kv_dim, seq_len = cache_ref.shape[2], cache_ref.shape[3]
    groups = toks // 8
    max_n = seq_len // CHUNK

    def group_n(g):
        return lax.div(slen_ref[g * 8] + (CHUNK - 1), CHUNK)

    def start_group(g):
        slot = lax.rem(g, slots)
        n = group_n(g)
        for k in range(max_n):
            @pl.when(k < n)
            def _():
                for i in range(8):
                    b = order_ref[g * 8 + i]
                    pltpu.make_async_copy(
                        cache_ref.at[layer, b, :, pl.ds(k * CHUNK, CHUNK)],
                        buf.at[slot, i // 4, k, pl.ds((i % 4) * kv_dim, kv_dim)], sem.at[slot]).start()

    wq_copy = pltpu.make_async_copy(wq_hbm.at[layer], wq, wsem.at[0])
    wo_copy = pltpu.make_async_copy(wo_hbm.at[layer], wo, wsem.at[1])
    wq_copy.start()
    x_copy = pltpu.make_async_copy(x_in, xbuf, wsem.at[2])
    if layer == 0:
        x_copy.start()
    x_ref = xbuf if layer == 0 else x_in
    lax.fori_loop(0, slots, lambda g, c: (start_group(g), c)[1], 0)
    wo_copy.start()

    rows = 2 * toks
    row_id = lax.broadcasted_iota(jnp.int32, (rows, toks), 0)
    place = place_ref[...]
    base = lax.shift_right_logical(place, 2) * 8 + lax.rem(place, 4)
    pick0 = (row_id == base).astype(BF16)
    pick1 = (row_id == base + 4).astype(BF16)
    if layer == 0:
        x_copy.wait()
    h = rms_norm(x_ref[...]).astype(BF16)
    wq_copy.wait()
    q = jnp.dot(h, wq[...], preferred_element_type=F32).astype(BF16)
    qrows = (jnp.dot(pick0, q[:, :kv_dim], preferred_element_type=F32)
             + jnp.dot(pick1, q[:, kv_dim:], preferred_element_type=F32))
    sub = lax.rem(lax.broadcasted_iota(jnp.int32, (rows, 1), 0), 4)
    twice = jnp.concatenate([qrows, qrows], axis=1)
    second = (lax.broadcasted_iota(jnp.int32, (rows, 2 * kv_dim), 1) >= kv_dim).astype(jnp.int32)
    for jj in range(2):
        lhs = jnp.where(sub == 2 * jj + second, twice, 0.0).astype(BF16)
        for t in range(2 * kv_dim // CHUNK):
            qbd[jj * (2 * kv_dim // CHUNK) + t] = lhs[:, t * CHUNK:(t + 1) * CHUNK]

    row16 = lax.broadcasted_iota(jnp.int32, (16, CHUNK), 0)
    sub16 = lax.rem(row16, 4)
    lane16 = lax.broadcasted_iota(jnp.int32, (16, CHUNK), 1)
    half16 = (row16 >= 8).astype(jnp.int32)
    seq16 = half16 * 4 + sub16

    def scores(g, nn):
        slot = lax.rem(g, slots)
        at16 = pl.ds(pl.multiple_of(g * 16, 16), 16)
        lhs = jnp.concatenate([qbd[t, at16, :] for t in range(qbd.shape[0])], axis=1)
        lens = jnp.zeros((16, CHUNK), jnp.int32)
        for i in range(8):
            lens = jnp.where(seq16 == i, slen_ref[g * 8 + i], lens)
        out = []
        for k in range(nn):
            rhs = jnp.concatenate([buf[slot, 0, k], buf[slot, 1, k]], axis=1)
            raw = jnp.dot(lhs, rhs, preferred_element_type=F32)
            s = jnp.concatenate([raw[0:8, :CHUNK], raw[8:16, CHUNK:]], axis=0) * ATT_SCALE
            out.append(jnp.where(lane16 + k * CHUNK < lens, s, -jnp.inf))
        return out

    def softmax(s):
        m = s[0]
        for t in s[1:]:
            m = jnp.maximum(m, t)
        m = jnp.max(m, axis=1, keepdims=True)
        e = [jnp.exp(t - m) for t in s]
        tot = e[0]
        for t in e[1:]:
            tot = tot + t
        inv = 1.0 / jnp.sum(tot, axis=1, keepdims=True)
        return [(t * inv) for t in e]

    def values(g, p):
        slot = lax.rem(g, slots)
        lhs, rhs = [], []
        for k, t in enumerate(p):
            for j in range(4):
                for half in range(2):
                    keep = (sub16 == j) & (half16 == half)
                    lhs.append(jnp.where(keep, t, 0.0).astype(BF16))
                    rhs.append(buf[slot, half, k, pl.ds(j * kv_dim, LATENT)])
        o = lax.dot_general(jnp.concatenate(lhs, axis=1), jnp.concatenate(rhs, axis=1),
                            (((1,), (1,)), ((), ())), preferred_element_type=F32)
        obuf[pl.ds(pl.multiple_of(g * 16, 16), 16), :] = o.astype(BF16)

    def wait_group(g, nn):
        slot = lax.rem(g, slots)
        view = buf.at[slot, :, pl.ds(0, nn)]
        pltpu.make_async_copy(view, view, sem.at[slot]).wait()

    def put_scores(g, nn):
        for k, t in enumerate(scores(g, nn)):
            pbuf[lax.rem(g, 2), k] = t

    def put_values(g, nn):
        values(g, softmax([pbuf[lax.rem(g, 2), k] for k in range(nn)]))

    def each_n(n, fn):
        for nn in range(1, max_n + 1):
            pl.when(n == nn)(functools.partial(fn, nn))

    def first(nn):
        wait_group(0, nn)
    each_n(group_n(0), first)
    put_scores(0, max_n)

    def body(g, _):
        each_n(group_n(g), functools.partial(wait_group, g))

        def both(nn):
            raw_prev = [pbuf[lax.rem(g - 1, 2), k] for k in range(nn)]
            s = scores(g, nn)
            values(g - 1, softmax(raw_prev))
            for k, t in enumerate(s):
                pbuf[lax.rem(g, 2), k] = t
        each_n(group_n(g - 1), both)

        @pl.when(g - 1 + slots < groups)
        def _():
            start_group(g - 1 + slots)
        return 0

    lax.fori_loop(1, groups, body, 0)
    each_n(group_n(groups - 1), functools.partial(put_values, groups - 1))

    wo_copy.wait()
    picked = obuf[...]
    total = x_ref[...].astype(F32)
    for head, pick in enumerate((pick0, pick1)):
        o = lax.dot_general(pick, picked, (((0,), (0,)), ((), ())), preferred_element_type=F32).astype(BF16)
        total = total + jnp.dot(o, wo[head * LATENT:(head + 1) * LATENT, :], preferred_element_type=F32)
    x_new = total.astype(BF16)
    x_out[...] = x_new
    g_out[...] = rms_norm(x_new).astype(BF16)


def attention(layer, place, order, sorted_len, x, cache_t, w_q, w_o, slots=8):
    toks, d_model = x.shape
    kv_dim, seq_len = cache_t.shape[2], cache_t.shape[3]
    any_spec = pl.BlockSpec(memory_space=pltpu.HBM)
    if layer == 0:
        x, w_q, w_o = (pltpu.with_memory_space_constraint(a, pltpu.HBM) for a in (x, w_q, w_o))
    smem = pl.BlockSpec(memory_space=pltpu.SMEM)
    vmem = pl.BlockSpec(memory_space=pltpu.VMEM)
    return pl.pallas_call(
        functools.partial(attn_kernel, layer, slots),
        out_shape=(jax.ShapeDtypeStruct((toks, d_model), BF16), jax.ShapeDtypeStruct((toks, d_model), BF16)),
        in_specs=[smem, smem, vmem, any_spec if layer == 0 else vmem, any_spec, any_spec, any_spec],
        out_specs=(vmem, vmem),
        scratch_shapes=[
            pltpu.VMEM(w_q.shape[1:], BF16),
            pltpu.VMEM(w_o.shape[1:], BF16),
            pltpu.VMEM((slots, 2, seq_len // CHUNK, 4 * kv_dim, CHUNK), BF16),
            pltpu.VMEM((4 * kv_dim // CHUNK, 2 * toks, CHUNK), BF16),
            pltpu.VMEM((2 * toks, LATENT), BF16),
            pltpu.VMEM((2, seq_len // CHUNK, 16, CHUNK), F32),
            pltpu.SemaphoreType.DMA((slots,)),
            pltpu.SemaphoreType.DMA((3,)),
            pltpu.VMEM((toks, d_model), BF16),
        ],
        compiler_params=pltpu.CompilerParams(vmem_limit_bytes=48 * 1024 * 1024),
        name="latent_attention",
    )(order, sorted_len, place.reshape(1, toks), x, cache_t, w_q, w_o)


MESH_ID = pl.DeviceIdType.MESH
EXP_STEP = 4


def moe_kernel(layer, x_ref, g_ref, ids_ref, slot_ref, gate_ref, w1, w3, w2, w1s, w3s, w2s, out_ref,
               gall, wall, route_ref, w2t, acc, part, gsend, grecv, rsend, rrecv, psend, precv):
    me = lax.axis_index('dp')
    core = lax.rem(me, 2)
    chip = lax.div(me, 2)
    partner = chip * 2 + (1 - core)
    cross = (1 - chip) * 2 + (1 - core)
    same = (1 - chip) * 2 + core
    peers = (partner, cross, same)
    _, experts, ff, d_model = w2.shape
    toks = x_ref.shape[0]

    expert_id = lax.broadcasted_iota(jnp.int32, route_ref.shape, 0)
    route = jnp.zeros(route_ref.shape, F32)
    for j in range(ids_ref.shape[0]):
        hit = (ids_ref[j, layer:layer + 1, :] == expert_id) & (slot_ref[j, layer:layer + 1, :] >= 0)
        route = route + jnp.where(hit, gate_ref[j, layer:layer + 1, :], 0.0)
    route_ref[...] = route

    barrier = pltpu.get_barrier_semaphore()
    for p in peers:
        pl.semaphore_signal(barrier, inc=1, device_id={'dp': p}, device_id_type=MESH_ID)
    pl.semaphore_wait(barrier, 3)

    gcopies, rcopies = [], []
    for i, p in enumerate(peers):
        rcopies.append(pltpu.make_async_remote_copy(
            route_ref.at[pl.ds(p * experts, experts)], wall.at[i + 1], rsend.at[i], rrecv.at[i],
            device_id={'dp': p}, device_id_type=MESH_ID))
        gcopies.append(pltpu.make_async_remote_copy(
            g_ref, gall.at[i + 1], gsend.at[i], grecv.at[i], device_id={'dp': p}, device_id_type=MESH_ID))
    for i in range(3):
        rcopies[i].start()
        gcopies[i].start()

    gall[0] = g_ref[...]
    wall[0] = route_ref[pl.ds(pl.multiple_of(me * experts, experts), experts), :]

    def flip(e, carry):
        w2t[e] = w2[layer, e].T
        return carry
    lax.fori_loop(0, experts, flip, 0)
    w2st = w2s[layer].T

    def gated(w3_rows, w1_rows, tok):
        dims = (((1,), (1,)), ((), ()))
        gate = lax.dot_general(w3_rows, tok, dims, preferred_element_type=F32)
        up = lax.dot_general(w1_rows, tok, dims, preferred_element_type=F32)
        return (gate * (1.0 / (1.0 + jnp.exp(-gate))) * up).astype(BF16)

    def ffn(blocks):
        tok = jnp.concatenate([gall[b] for b in blocks], axis=0)
        first = jnp.dot(w2st, gated(w3s[layer], w1s[layer], tok), preferred_element_type=F32)
        for n, b in enumerate(blocks):
            acc[b] = first[:, n * toks:(n + 1) * toks]

        def step(s, carry):
            rows = slice(s * EXP_STEP * ff, (s + 1) * EXP_STEP * ff)
            hid = gated(w3[layer, rows, :], w1[layer, rows, :], tok)
            total = [acc[b] for b in blocks]
            for i in range(EXP_STEP):
                e = s * EXP_STEP + i
                u = jnp.dot(w2t[e], hid[i * ff:(i + 1) * ff], preferred_element_type=F32)
                u = u.astype(BF16).astype(F32)
                for n, b in enumerate(blocks):
                    w = wall[b, e:e + 1, :]
                    total[n] = total[n] + jnp.where(w > 0.0, u[:, n * toks:(n + 1) * toks] * w, 0.0)
            for n, b in enumerate(blocks):
                acc[b] = total[n]
            return carry
        for s in range(experts // EXP_STEP):
            step(s, 0)

    def send_part(i, src, dst_ref, dst):
        return pltpu.make_async_remote_copy(
            src, dst_ref, psend.at[i], precv.at[i], device_id={'dp': dst}, device_id_type=MESH_ID)

    rcopies[0].wait_recv()
    gcopies[0].wait_recv()
    ffn((0, 1))
    home = send_part(0, acc.at[1], part.at[0], partner)
    home.start()

    rcopies[1].wait_recv()
    gcopies[1].wait_recv()
    ffn((2,))
    relay = send_part(1, acc.at[2], part.at[1], partner)
    relay.start()

    rcopies[2].wait_recv()
    gcopies[2].wait_recv()
    ffn((3,))
    relay.wait_recv()
    half = d_model // 2
    far = []
    for i in range(2):
        rows = slice(i * half, (i + 1) * half)
        acc[4, rows] = acc[3, rows] + part[1, rows]
        at = pl.ds(i * half, half)
        far.append(send_part(2 + i, acc.at[4, at], part.at[2, at], same))
        far[i].start()
    home.wait_recv()
    acc[0] = acc[0] + part[0]
    for i in range(2):
        rows = slice(i * half, (i + 1) * half)
        far[i].wait_recv()
        out_ref[:, rows] = (x_ref[:, rows].astype(F32) + (acc[0, rows] + part[2, rows]).T).astype(BF16)

    for c in gcopies + rcopies + [home, relay] + far:
        c.wait_send()


def moe(layer, x, g, ids, slot, gate, total_experts, w1, w3, w2, w1s, w3s, w2s):
    toks, d_model = x.shape
    _, experts, ff, _ = w2.shape
    vmem = pl.BlockSpec(memory_space=pltpu.VMEM)
    dma = pltpu.SemaphoreType.DMA
    return pl.pallas_call(
        functools.partial(moe_kernel, layer),
        out_shape=jax.ShapeDtypeStruct((toks, d_model), BF16),
        in_specs=[vmem] * 11,
        out_specs=vmem,
        scratch_shapes=[
            pltpu.VMEM((4, toks, d_model), BF16),
            pltpu.VMEM((4, experts, toks), F32),
            pltpu.VMEM((total_experts, toks), F32),
            pltpu.VMEM((experts, d_model, ff), BF16),
            pltpu.VMEM((5, d_model, toks), F32),
            pltpu.VMEM((3, d_model, toks), F32),
            dma((3,)), dma((3,)), dma((3,)), dma((3,)), dma((4,)), dma((4,)),
        ],
        compiler_params=pltpu.CompilerParams(
            collective_id=layer, has_side_effects=True, vmem_limit_bytes=40 * 1024 * 1024),
        name="expert_exchange",
    )(x, g, ids, slot, gate, w1, w3, w2, w1s, w3s, w2s)


def solution(mesh):
    tok_axes = ('replica', 'dp')
    in_specs = (
        P(tok_axes, None), P(tok_axes), P(None, tok_axes, None, None),
        P(None, None, None), P(None, None, None),
        P(None, tok_axes, None), P(None, tok_axes, None), P(None, tok_axes, None),
        P(None, 'dp', None, None), P(None, 'dp', None, None), P(None, 'dp', None, None),
        P(None, None, 'dp'), P(None, None, 'dp'), P(None, 'dp', None),
    )

    def device_step(x, lengths, cache, w_q, w_o, expert_ids, slots, route_w, w1_exp, w3_exp, w2_exp, w1_sh, w3_sh, w2_sh):
        layers, local, d_model, ff = w1_exp.shape
        place, order, sorted_len = bucket_order(lengths)
        cache_t = jnp.swapaxes(cache, 2, 3)
        by_choice = [jnp.transpose(a, (2, 0, 1)) for a in (expert_ids, slots, route_w)]
        w1 = jnp.swapaxes(w1_exp, 2, 3).reshape(layers, local * ff, d_model)
        w3 = jnp.swapaxes(w3_exp, 2, 3).reshape(layers, local * ff, d_model)
        w1s, w3s = jnp.swapaxes(w1_sh, 1, 2), jnp.swapaxes(w3_sh, 1, 2)
        experts = local * mesh.shape['dp']
        resid = x
        for layer in range(layers):
            resid, ffn_in = attention(layer, place, order, sorted_len, resid, cache_t, w_q, w_o)
            resid = moe(layer, resid, ffn_in, *by_choice, experts, w1, w3, w2_exp, w1s, w3s, w2_sh)
        return resid

    return jax.shard_map(device_step, mesh=mesh, in_specs=in_specs, out_specs=P(tok_axes, None), check_vma=False)
```

```python
import functools
import jax
import jax.numpy as jnp
from jax import lax
from jax.experimental import pallas as pl
from jax.experimental.pallas import tpu as pltpu
from jax.sharding import PartitionSpec as P

NORM_EPS = 1e-6
ATT_SCALE = 1.0 / (192.0 ** 0.5)
LATENT = 512
CHUNK = 128
F32 = jnp.float32
MXU_COLS = 256
VBLK = 64
BF16 = jnp.bfloat16


def rms_norm(values):
    vals32 = values.astype(F32)
    return vals32 * lax.rsqrt(jnp.mean(vals32 * vals32, axis=-1, keepdims=True) + NORM_EPS)


def bucket_order(lengths):
    count = lengths.shape[0]
    chunks = (lengths + (CHUNK - 1)) // CHUNK
    ids = jnp.arange(count, dtype=jnp.int32)
    ahead = (chunks[None, :] > chunks[:, None]) | ((chunks[None, :] == chunks[:, None]) & (ids[None, :] < ids[:, None]))
    place = jnp.sum(ahead.astype(jnp.int32), axis=1)
    hit = place[None, :] == ids[:, None]
    order = jnp.sum(jnp.where(hit, ids[None, :], 0), axis=1)
    sorted_len = jnp.sum(jnp.where(hit, lengths[None, :], 0), axis=1)
    return place, order, sorted_len


def attn_kernel(layer, slots, order_ref, slen_ref, place_ref, x_in, cache_ref, wq_hbm, wo_hbm,
                x_out, g_out, wq, wo, buf, qbd, obuf, pbuf, sem, wsem, xbuf):
    toks, d_model = x_in.shape
    kv_dim, seq_len = cache_ref.shape[2], cache_ref.shape[3]
    groups = toks // 8
    max_n = seq_len // CHUNK

    def group_n(g):
        return lax.div(slen_ref[g * 8] + (CHUNK - 1), CHUNK)

    def start_group(g):
        slot = lax.rem(g, slots)
        n = group_n(g)
        for nn in range(1, max_n + 1):
            @pl.when(n == nn)
            def _():
                cols = pl.ds(0, nn * CHUNK)
                for i in range(8):
                    b = order_ref[g * 8 + i]
                    pltpu.make_async_copy(
                        cache_ref.at[layer, b, :, cols],
                        buf.at[slot, i // 4, pl.ds((i % 4) * kv_dim, kv_dim), cols], sem.at[slot]).start()

    wq_copy = pltpu.make_async_copy(wq_hbm.at[layer], wq, wsem.at[0])
    wo_copy = pltpu.make_async_copy(wo_hbm.at[layer], wo, wsem.at[1])
    wq_copy.start()
    x_copy = pltpu.make_async_copy(x_in, xbuf, wsem.at[2])
    if layer == 0:
        x_copy.start()
    x_ref = xbuf if layer == 0 else x_in
    lax.fori_loop(0, slots, lambda g, c: (start_group(g), c)[1], 0)
    wo_copy.start()

    rows = 2 * toks
    row_id = lax.broadcasted_iota(jnp.int32, (rows, toks), 0)
    place = place_ref[...]
    base = lax.shift_right_logical(place, 2) * 8 + lax.rem(place, 4)
    pick0 = (row_id == base).astype(BF16)
    pick1 = (row_id == base + 4).astype(BF16)
    if layer == 0:
        x_copy.wait()
    h = rms_norm(x_ref[...]).astype(BF16)
    wq_copy.wait()
    q = jnp.dot(h, wq[...], preferred_element_type=F32).astype(BF16)
    qrows = (jnp.dot(pick0, q[:, :kv_dim], preferred_element_type=F32)
             + jnp.dot(pick1, q[:, kv_dim:], preferred_element_type=F32))
    sub = lax.rem(lax.broadcasted_iota(jnp.int32, (rows, 1), 0), 4)
    twice = jnp.concatenate([qrows, qrows], axis=1)
    second = (lax.broadcasted_iota(jnp.int32, (rows, 2 * kv_dim), 1) >= kv_dim).astype(jnp.int32)
    for jj in range(2):
        lhs = jnp.where(sub == 2 * jj + second, twice, 0.0).astype(BF16)
        for t in range(2 * kv_dim // CHUNK):
            qbd[jj * (2 * kv_dim // CHUNK) + t] = lhs[:, t * CHUNK:(t + 1) * CHUNK]

    row16 = lax.broadcasted_iota(jnp.int32, (16, CHUNK), 0)
    sub16 = lax.rem(row16, 4)
    lane16 = lax.broadcasted_iota(jnp.int32, (16, CHUNK), 1)
    half16 = (row16 >= 8).astype(jnp.int32)
    seq16 = half16 * 4 + sub16

    def scores(g, nn):
        slot = lax.rem(g, slots)
        at16 = pl.ds(pl.multiple_of(g * 16, 16), 16)
        lhs = jnp.concatenate([qbd[t, at16, :] for t in range(qbd.shape[0])], axis=1)
        lens = jnp.zeros((16, CHUNK), jnp.int32)
        for i in range(8):
            lens = jnp.where(seq16 == i, slen_ref[g * 8 + i], lens)
        out = []
        for k in range(nn):
            cols = pl.ds(k * CHUNK, CHUNK)
            rhs = jnp.concatenate([buf[slot, 0, :, cols], buf[slot, 1, :, cols]], axis=1)
            raw = jnp.dot(lhs, rhs, preferred_element_type=F32)
            s = jnp.concatenate([raw[0:8, :CHUNK], raw[8:16, CHUNK:]], axis=0) * ATT_SCALE
            out.append(jnp.where(lane16 + k * CHUNK < lens, s, -jnp.inf))
        return out

    def softmax(s):
        m = s[0]
        for t in s[1:]:
            m = jnp.maximum(m, t)
        m = jnp.max(m, axis=1, keepdims=True)
        e = [jnp.exp(t - m) for t in s]
        tot = e[0]
        for t in e[1:]:
            tot = tot + t
        inv = 1.0 / jnp.sum(tot, axis=1, keepdims=True)
        return [(t * inv) for t in e]

    lane_blk = lax.broadcasted_iota(jnp.int32, (VBLK, CHUNK), 1)

    def values(g, p):
        slot = lax.rem(g, slots)
        at16 = pl.ds(pl.multiple_of(g * 16, 16), 16)
        lhs, rhs = [], []
        for k, t in enumerate(p):
            for j in range(4):
                for half in range(2):
                    keep = (sub16 == j) & (half16 == half)
                    lhs.append(jnp.where(keep, t, 0.0).astype(BF16))
                    rhs.append(buf[slot, half, pl.ds(j * kv_dim, MXU_COLS), pl.ds(k * CHUNK, CHUNK)])
        o = lax.dot_general(jnp.concatenate(lhs, axis=1), jnp.concatenate(rhs, axis=1),
                            (((1,), (1,)), ((), ())), preferred_element_type=F32)
        obuf[at16, :MXU_COLS] = o.astype(BF16)
        rounded = [t.astype(BF16).astype(F32) for t in p]
        blocks = (LATENT - MXU_COLS) // VBLK
        picked = [jnp.zeros((VBLK, CHUNK), F32) for _ in range(blocks)]
        for half in range(2):
            for j in range(4):
                for c in range(blocks):
                    sums = [None, None]
                    for k in range(len(p)):
                        tile = buf[slot, half, pl.ds(j * kv_dim + MXU_COLS + c * VBLK, VBLK), pl.ds(k * CHUNK, CHUNK)].astype(F32)
                        for head in range(2):
                            row = half * 8 + head * 4 + j
                            term = tile * rounded[k][row:row + 1, :]
                            sums[head] = term if k == 0 else sums[head] + term
                    for head in range(2):
                        row = half * 8 + head * 4 + j
                        picked[c] = jnp.where(lane_blk == row, jnp.sum(sums[head], axis=1, keepdims=True), picked[c])
        obuf[at16, MXU_COLS:] = jnp.concatenate(picked, axis=0).T[:16].astype(BF16)

    def wait_group(g, nn):
        slot = lax.rem(g, slots)
        view = buf.at[slot, :, :, pl.ds(0, nn * CHUNK)]
        pltpu.make_async_copy(view, view, sem.at[slot]).wait()

    def put_scores(g, nn):
        for k, t in enumerate(scores(g, nn)):
            pbuf[lax.rem(g, 2), k] = t

    def put_values(g, nn):
        values(g, softmax([pbuf[lax.rem(g, 2), k] for k in range(nn)]))

    def each_n(n, fn):
        for nn in range(1, max_n + 1):
            pl.when(n == nn)(functools.partial(fn, nn))

    def first(nn):
        wait_group(0, nn)
    each_n(group_n(0), first)
    put_scores(0, max_n)

    def body(g, _):
        each_n(group_n(g), functools.partial(wait_group, g))

        def both(nn):
            raw_prev = [pbuf[lax.rem(g - 1, 2), k] for k in range(nn)]
            s = scores(g, nn)
            values(g - 1, softmax(raw_prev))
            for k, t in enumerate(s):
                pbuf[lax.rem(g, 2), k] = t
        each_n(group_n(g - 1), both)

        @pl.when(g - 1 + slots < groups)
        def _():
            start_group(g - 1 + slots)
        return 0

    lax.fori_loop(1, groups, body, 0)
    each_n(group_n(groups - 1), functools.partial(put_values, groups - 1))

    wo_copy.wait()
    picked = obuf[...]
    total = x_ref[...].astype(F32)
    for head, pick in enumerate((pick0, pick1)):
        o = lax.dot_general(pick, picked, (((0,), (0,)), ((), ())), preferred_element_type=F32).astype(BF16)
        total = total + jnp.dot(o, wo[head * LATENT:(head + 1) * LATENT, :], preferred_element_type=F32)
    x_new = total.astype(BF16)
    x_out[...] = x_new
    g_out[...] = rms_norm(x_new).astype(BF16)


def attention(layer, place, order, sorted_len, x, cache_t, w_q, w_o, slots=8):
    toks, d_model = x.shape
    kv_dim, seq_len = cache_t.shape[2], cache_t.shape[3]
    any_spec = pl.BlockSpec(memory_space=pltpu.HBM)
    if layer == 0:
        x, w_q, w_o = (pltpu.with_memory_space_constraint(a, pltpu.HBM) for a in (x, w_q, w_o))
    smem = pl.BlockSpec(memory_space=pltpu.SMEM)
    vmem = pl.BlockSpec(memory_space=pltpu.VMEM)
    return pl.pallas_call(
        functools.partial(attn_kernel, layer, slots),
        out_shape=(jax.ShapeDtypeStruct((toks, d_model), BF16), jax.ShapeDtypeStruct((toks, d_model), BF16)),
        in_specs=[smem, smem, vmem, any_spec if layer == 0 else vmem, any_spec, any_spec, any_spec],
        out_specs=(vmem, vmem),
        scratch_shapes=[
            pltpu.VMEM(w_q.shape[1:], BF16),
            pltpu.VMEM(w_o.shape[1:], BF16),
            pltpu.VMEM((slots, 2, 4 * kv_dim, seq_len), BF16),
            pltpu.VMEM((4 * kv_dim // CHUNK, 2 * toks, CHUNK), BF16),
            pltpu.VMEM((2 * toks, LATENT), BF16),
            pltpu.VMEM((2, seq_len // CHUNK, 16, CHUNK), F32),
            pltpu.SemaphoreType.DMA((slots,)),
            pltpu.SemaphoreType.DMA((3,)),
            pltpu.VMEM((toks, d_model), BF16),
        ],
        compiler_params=pltpu.CompilerParams(vmem_limit_bytes=48 * 1024 * 1024),
        name="latent_attention",
    )(order, sorted_len, place.reshape(1, toks), x, cache_t, w_q, w_o)


MESH_ID = pl.DeviceIdType.MESH
EXP_STEP = 4


def moe_kernel(layer, x_ref, g_ref, ids_ref, slot_ref, gate_ref, w1, w3, w2, w1s, w3s, w2s, out_ref,
               gall, wall, route_ref, w2t, acc, part, gsend, grecv, rsend, rrecv, psend, precv):
    me = lax.axis_index('dp')
    core = lax.rem(me, 2)
    chip = lax.div(me, 2)
    partner = chip * 2 + (1 - core)
    cross = (1 - chip) * 2 + (1 - core)
    same = (1 - chip) * 2 + core
    peers = (partner, cross, same)
    _, experts, ff, d_model = w2.shape
    toks = x_ref.shape[0]

    expert_id = lax.broadcasted_iota(jnp.int32, route_ref.shape, 0)
    route = jnp.zeros(route_ref.shape, F32)
    for j in range(ids_ref.shape[0]):
        hit = (ids_ref[j, layer:layer + 1, :] == expert_id) & (slot_ref[j, layer:layer + 1, :] >= 0)
        route = route + jnp.where(hit, gate_ref[j, layer:layer + 1, :], 0.0)
    route_ref[...] = route

    barrier = pltpu.get_barrier_semaphore()
    for p in peers:
        pl.semaphore_signal(barrier, inc=1, device_id={'dp': p}, device_id_type=MESH_ID)
    pl.semaphore_wait(barrier, 3)

    gcopies, rcopies = [], []
    for i, p in enumerate(peers):
        rcopies.append(pltpu.make_async_remote_copy(
            route_ref.at[pl.ds(p * experts, experts)], wall.at[i + 1], rsend.at[i], rrecv.at[i],
            device_id={'dp': p}, device_id_type=MESH_ID))
        gcopies.append(pltpu.make_async_remote_copy(
            g_ref, gall.at[i + 1], gsend.at[i], grecv.at[i], device_id={'dp': p}, device_id_type=MESH_ID))
    for i in range(3):
        rcopies[i].start()
        gcopies[i].start()

    gall[0] = g_ref[...]
    wall[0] = route_ref[pl.ds(pl.multiple_of(me * experts, experts), experts), :]

    def flip(e, carry):
        w2t[e] = w2[layer, e].T
        return carry
    lax.fori_loop(0, experts, flip, 0)
    w2st = w2s[layer].T

    def gated(w3_rows, w1_rows, tok):
        dims = (((1,), (1,)), ((), ()))
        gate = lax.dot_general(w3_rows, tok, dims, preferred_element_type=F32)
        up = lax.dot_general(w1_rows, tok, dims, preferred_element_type=F32)
        return (gate * (1.0 / (1.0 + jnp.exp(-gate))) * up).astype(BF16)

    def ffn(blocks):
        tok = jnp.concatenate([gall[b] for b in blocks], axis=0)
        first = jnp.dot(w2st, gated(w3s[layer], w1s[layer], tok), preferred_element_type=F32)
        for n, b in enumerate(blocks):
            acc[b] = first[:, n * toks:(n + 1) * toks]

        def step(s, carry):
            rows = slice(s * EXP_STEP * ff, (s + 1) * EXP_STEP * ff)
            hid = gated(w3[layer, rows, :], w1[layer, rows, :], tok)
            total = [acc[b] for b in blocks]
            for i in range(EXP_STEP):
                e = s * EXP_STEP + i
                u = jnp.dot(w2t[e], hid[i * ff:(i + 1) * ff], preferred_element_type=F32)
                u = u.astype(BF16).astype(F32)
                for n, b in enumerate(blocks):
                    w = wall[b, e:e + 1, :]
                    total[n] = total[n] + jnp.where(w > 0.0, u[:, n * toks:(n + 1) * toks] * w, 0.0)
            for n, b in enumerate(blocks):
                acc[b] = total[n]
            return carry
        for s in range(experts // EXP_STEP):
            step(s, 0)

    def send_part(i, src, dst_ref, dst):
        return pltpu.make_async_remote_copy(
            src, dst_ref, psend.at[i], precv.at[i], device_id={'dp': dst}, device_id_type=MESH_ID)

    rcopies[0].wait_recv()
    gcopies[0].wait_recv()
    ffn((0, 1))
    home = send_part(0, acc.at[1], part.at[0], partner)
    home.start()

    rcopies[1].wait_recv()
    gcopies[1].wait_recv()
    ffn((2,))
    relay = send_part(1, acc.at[2], part.at[1], partner)
    relay.start()

    rcopies[2].wait_recv()
    gcopies[2].wait_recv()
    ffn((3,))
    relay.wait_recv()
    half = d_model // 2
    far = []
    for i in range(2):
        rows = slice(i * half, (i + 1) * half)
        acc[4, rows] = acc[3, rows] + part[1, rows]
        at = pl.ds(i * half, half)
        far.append(send_part(2 + i, acc.at[4, at], part.at[2, at], same))
        far[i].start()
    home.wait_recv()
    acc[0] = acc[0] + part[0]
    for i in range(2):
        rows = slice(i * half, (i + 1) * half)
        far[i].wait_recv()
        out_ref[:, rows] = (x_ref[:, rows].astype(F32) + (acc[0, rows] + part[2, rows]).T).astype(BF16)

    for c in gcopies + rcopies + [home, relay] + far:
        c.wait_send()


def moe(layer, x, g, ids, slot, gate, total_experts, w1, w3, w2, w1s, w3s, w2s):
    toks, d_model = x.shape
    _, experts, ff, _ = w2.shape
    vmem = pl.BlockSpec(memory_space=pltpu.VMEM)
    dma = pltpu.SemaphoreType.DMA
    return pl.pallas_call(
        functools.partial(moe_kernel, layer),
        out_shape=jax.ShapeDtypeStruct((toks, d_model), BF16),
        in_specs=[vmem] * 11,
        out_specs=vmem,
        scratch_shapes=[
            pltpu.VMEM((4, toks, d_model), BF16),
            pltpu.VMEM((4, experts, toks), F32),
            pltpu.VMEM((total_experts, toks), F32),
            pltpu.VMEM((experts, d_model, ff), BF16),
            pltpu.VMEM((5, d_model, toks), F32),
            pltpu.VMEM((3, d_model, toks), F32),
            dma((3,)), dma((3,)), dma((3,)), dma((3,)), dma((4,)), dma((4,)),
        ],
        compiler_params=pltpu.CompilerParams(
            collective_id=layer, has_side_effects=True, vmem_limit_bytes=40 * 1024 * 1024),
        name="expert_exchange",
    )(x, g, ids, slot, gate, w1, w3, w2, w1s, w3s, w2s)


def solution(mesh):
    tok_axes = ('replica', 'dp')
    in_specs = (
        P(tok_axes, None), P(tok_axes), P(None, tok_axes, None, None),
        P(None, None, None), P(None, None, None),
        P(None, tok_axes, None), P(None, tok_axes, None), P(None, tok_axes, None),
        P(None, 'dp', None, None), P(None, 'dp', None, None), P(None, 'dp', None, None),
        P(None, None, 'dp'), P(None, None, 'dp'), P(None, 'dp', None),
    )

    def device_step(x, lengths, cache, w_q, w_o, expert_ids, slots, route_w, w1_exp, w3_exp, w2_exp, w1_sh, w3_sh, w2_sh):
        layers, local, d_model, ff = w1_exp.shape
        place, order, sorted_len = bucket_order(lengths)
        cache_t = jnp.swapaxes(cache, 2, 3)
        by_choice = [jnp.transpose(a, (2, 0, 1)) for a in (expert_ids, slots, route_w)]
        w1 = jnp.swapaxes(w1_exp, 2, 3).reshape(layers, local * ff, d_model)
        w3 = jnp.swapaxes(w3_exp, 2, 3).reshape(layers, local * ff, d_model)
        w1s, w3s = jnp.swapaxes(w1_sh, 1, 2), jnp.swapaxes(w3_sh, 1, 2)
        experts = local * mesh.shape['dp']
        resid = x
        for layer in range(layers):
            resid, ffn_in = attention(layer, place, order, sorted_len, resid, cache_t, w_q, w_o)
            resid = moe(layer, resid, ffn_in, *by_choice, experts, w1, w3, w2_exp, w1s, w3s, w2_sh)
        return resid

    return jax.shard_map(device_step, mesh=mesh, in_specs=in_specs, out_specs=P(tok_axes, None), check_vma=False)
```

```python
import functools
import jax
import jax.numpy as jnp
from jax import lax
from jax.experimental import pallas as pl
from jax.experimental.pallas import tpu as pltpu
from jax.sharding import PartitionSpec as P

NORM_EPS = 1e-6
ATT_SCALE = 1.0 / (192.0 ** 0.5)
LATENT = 512
CHUNK = 128
F32 = jnp.float32
MXU_COLS = (512, 384, 256, 256)
VBLK = 64
BF16 = jnp.bfloat16


def rms_norm(values):
    vals32 = values.astype(F32)
    return vals32 * lax.rsqrt(jnp.mean(vals32 * vals32, axis=-1, keepdims=True) + NORM_EPS)


def bucket_order(lengths):
    count = lengths.shape[0]
    chunks = (lengths + (CHUNK - 1)) // CHUNK
    ids = jnp.arange(count, dtype=jnp.int32)
    ahead = (chunks[None, :] > chunks[:, None]) | ((chunks[None, :] == chunks[:, None]) & (ids[None, :] < ids[:, None]))
    place = jnp.sum(ahead.astype(jnp.int32), axis=1)
    hit = place[None, :] == ids[:, None]
    order = jnp.sum(jnp.where(hit, ids[None, :], 0), axis=1)
    sorted_len = jnp.sum(jnp.where(hit, lengths[None, :], 0), axis=1)
    return place, order, sorted_len


def attn_kernel(layer, slots, order_ref, slen_ref, place_ref, x_in, cache_ref, wq_hbm, wo_hbm,
                x_out, g_out, wq, wo, buf, qbd, obuf, pbuf, sem, wsem, xbuf):
    toks, d_model = x_in.shape
    kv_dim, seq_len = cache_ref.shape[2], cache_ref.shape[3]
    groups = toks // 8
    max_n = seq_len // CHUNK

    def group_n(g):
        return lax.div(slen_ref[g * 8] + (CHUNK - 1), CHUNK)

    def start_group(g):
        slot = lax.rem(g, slots)
        n = group_n(g)
        for nn in range(1, max_n + 1):
            @pl.when(n == nn)
            def _():
                cols = pl.ds(0, nn * CHUNK)
                for i in range(8):
                    b = order_ref[g * 8 + i]
                    pltpu.make_async_copy(
                        cache_ref.at[layer, b, :, cols],
                        buf.at[slot, i // 4, pl.ds((i % 4) * kv_dim, kv_dim), cols], sem.at[slot]).start()

    wq_copy = pltpu.make_async_copy(wq_hbm.at[layer], wq, wsem.at[0])
    wo_copy = pltpu.make_async_copy(wo_hbm.at[layer], wo, wsem.at[1])
    wq_copy.start()
    x_copy = pltpu.make_async_copy(x_in, xbuf, wsem.at[2])
    if layer == 0:
        x_copy.start()
    x_ref = xbuf if layer == 0 else x_in
    lax.fori_loop(0, slots, lambda g, c: (start_group(g), c)[1], 0)
    wo_copy.start()

    rows = 2 * toks
    row_id = lax.broadcasted_iota(jnp.int32, (rows, toks), 0)
    place = place_ref[...]
    base = lax.shift_right_logical(place, 2) * 8 + lax.rem(place, 4)
    pick0 = (row_id == base).astype(BF16)
    pick1 = (row_id == base + 4).astype(BF16)
    if layer == 0:
        x_copy.wait()
    h = rms_norm(x_ref[...]).astype(BF16)
    wq_copy.wait()
    q = jnp.dot(h, wq[...], preferred_element_type=F32).astype(BF16)
    qrows = (jnp.dot(pick0, q[:, :kv_dim], preferred_element_type=F32)
             + jnp.dot(pick1, q[:, kv_dim:], preferred_element_type=F32))
    sub = lax.rem(lax.broadcasted_iota(jnp.int32, (rows, 1), 0), 4)
    twice = jnp.concatenate([qrows, qrows], axis=1)
    second = (lax.broadcasted_iota(jnp.int32, (rows, 2 * kv_dim), 1) >= kv_dim).astype(jnp.int32)
    for jj in range(2):
        lhs = jnp.where(sub == 2 * jj + second, twice, 0.0).astype(BF16)
        for t in range(2 * kv_dim // CHUNK):
            qbd[jj * (2 * kv_dim // CHUNK) + t] = lhs[:, t * CHUNK:(t + 1) * CHUNK]

    row16 = lax.broadcasted_iota(jnp.int32, (16, CHUNK), 0)
    sub16 = lax.rem(row16, 4)
    lane16 = lax.broadcasted_iota(jnp.int32, (16, CHUNK), 1)
    half16 = (row16 >= 8).astype(jnp.int32)
    seq16 = half16 * 4 + sub16

    def scores(g, nn):
        slot = lax.rem(g, slots)
        at16 = pl.ds(pl.multiple_of(g * 16, 16), 16)
        lhs = jnp.concatenate([qbd[t, at16, :] for t in range(qbd.shape[0])], axis=1)
        lens = jnp.zeros((16, CHUNK), jnp.int32)
        for i in range(8):
            lens = jnp.where(seq16 == i, slen_ref[g * 8 + i], lens)
        out = []
        for k in range(nn):
            cols = pl.ds(k * CHUNK, CHUNK)
            rhs = jnp.concatenate([buf[slot, 0, :, cols], buf[slot, 1, :, cols]], axis=1)
            raw = jnp.dot(lhs, rhs, preferred_element_type=F32)
            s = jnp.concatenate([raw[0:8, :CHUNK], raw[8:16, CHUNK:]], axis=0) * ATT_SCALE
            out.append(jnp.where(lane16 + k * CHUNK < lens, s, -jnp.inf))
        return out

    def softmax(s):
        m = s[0]
        for t in s[1:]:
            m = jnp.maximum(m, t)
        m = jnp.max(m, axis=1, keepdims=True)
        e = [jnp.exp(t - m) for t in s]
        tot = e[0]
        for t in e[1:]:
            tot = tot + t
        inv = 1.0 / jnp.sum(tot, axis=1, keepdims=True)
        return [(t * inv) for t in e]

    lane_blk = lax.broadcasted_iota(jnp.int32, (VBLK, CHUNK), 1)

    def values(g, p):
        slot = lax.rem(g, slots)
        at16 = pl.ds(pl.multiple_of(g * 16, 16), 16)
        mxu_cols = MXU_COLS[len(p) - 1]
        lhs, rhs = [], []
        for k, t in enumerate(p):
            for j in range(4):
                for half in range(2):
                    keep = (sub16 == j) & (half16 == half)
                    lhs.append(jnp.where(keep, t, 0.0).astype(BF16))
                    rhs.append(buf[slot, half, pl.ds(j * kv_dim, mxu_cols), pl.ds(k * CHUNK, CHUNK)])
        o = lax.dot_general(jnp.concatenate(lhs, axis=1), jnp.concatenate(rhs, axis=1),
                            (((1,), (1,)), ((), ())), preferred_element_type=F32)
        obuf[at16, :mxu_cols] = o.astype(BF16)
        if mxu_cols == LATENT:
            return
        rounded = [t.astype(BF16).astype(F32) for t in p]
        blocks = (LATENT - mxu_cols) // VBLK
        picked = [jnp.zeros((VBLK, CHUNK), F32) for _ in range(blocks)]
        for half in range(2):
            for j in range(4):
                for c in range(blocks):
                    sums = [None, None]
                    for k in range(len(p)):
                        tile = buf[slot, half, pl.ds(j * kv_dim + mxu_cols + c * VBLK, VBLK), pl.ds(k * CHUNK, CHUNK)].astype(F32)
                        for head in range(2):
                            row = half * 8 + head * 4 + j
                            term = tile * rounded[k][row:row + 1, :]
                            sums[head] = term if k == 0 else sums[head] + term
                    for head in range(2):
                        row = half * 8 + head * 4 + j
                        picked[c] = jnp.where(lane_blk == row, jnp.sum(sums[head], axis=1, keepdims=True), picked[c])
        obuf[at16, mxu_cols:] = jnp.concatenate(picked, axis=0).T[:16].astype(BF16)

    def wait_group(g, nn):
        slot = lax.rem(g, slots)
        view = buf.at[slot, :, :, pl.ds(0, nn * CHUNK)]
        pltpu.make_async_copy(view, view, sem.at[slot]).wait()

    def put_scores(g, nn):
        for k, t in enumerate(scores(g, nn)):
            pbuf[lax.rem(g, 2), k] = t

    def put_values(g, nn):
        values(g, softmax([pbuf[lax.rem(g, 2), k] for k in range(nn)]))

    def each_n(n, fn):
        for nn in range(1, max_n + 1):
            pl.when(n == nn)(functools.partial(fn, nn))

    def first(nn):
        wait_group(0, nn)
    each_n(group_n(0), first)
    put_scores(0, max_n)

    def body(g, _):
        each_n(group_n(g), functools.partial(wait_group, g))

        def both(nn):
            raw_prev = [pbuf[lax.rem(g - 1, 2), k] for k in range(nn)]
            s = scores(g, nn)
            values(g - 1, softmax(raw_prev))
            for k, t in enumerate(s):
                pbuf[lax.rem(g, 2), k] = t
        each_n(group_n(g - 1), both)

        @pl.when(g - 1 + slots < groups)
        def _():
            start_group(g - 1 + slots)
        return 0

    lax.fori_loop(1, groups, body, 0)
    each_n(group_n(groups - 1), functools.partial(put_values, groups - 1))

    wo_copy.wait()
    picked = obuf[...]
    total = x_ref[...].astype(F32)
    for head, pick in enumerate((pick0, pick1)):
        o = lax.dot_general(pick, picked, (((0,), (0,)), ((), ())), preferred_element_type=F32).astype(BF16)
        total = total + jnp.dot(o, wo[head * LATENT:(head + 1) * LATENT, :], preferred_element_type=F32)
    x_new = total.astype(BF16)
    x_out[...] = x_new
    g_out[...] = rms_norm(x_new).astype(BF16)


def attention(layer, place, order, sorted_len, x, cache_t, w_q, w_o, slots=8):
    toks, d_model = x.shape
    kv_dim, seq_len = cache_t.shape[2], cache_t.shape[3]
    any_spec = pl.BlockSpec(memory_space=pltpu.HBM)
    if layer == 0:
        x, w_q, w_o = (pltpu.with_memory_space_constraint(a, pltpu.HBM) for a in (x, w_q, w_o))
    smem = pl.BlockSpec(memory_space=pltpu.SMEM)
    vmem = pl.BlockSpec(memory_space=pltpu.VMEM)
    return pl.pallas_call(
        functools.partial(attn_kernel, layer, slots),
        out_shape=(jax.ShapeDtypeStruct((toks, d_model), BF16), jax.ShapeDtypeStruct((toks, d_model), BF16)),
        in_specs=[smem, smem, vmem, any_spec if layer == 0 else vmem, any_spec, any_spec, any_spec],
        out_specs=(vmem, vmem),
        scratch_shapes=[
            pltpu.VMEM(w_q.shape[1:], BF16),
            pltpu.VMEM(w_o.shape[1:], BF16),
            pltpu.VMEM((slots, 2, 4 * kv_dim, seq_len), BF16),
            pltpu.VMEM((4 * kv_dim // CHUNK, 2 * toks, CHUNK), BF16),
            pltpu.VMEM((2 * toks, LATENT), BF16),
            pltpu.VMEM((2, seq_len // CHUNK, 16, CHUNK), F32),
            pltpu.SemaphoreType.DMA((slots,)),
            pltpu.SemaphoreType.DMA((3,)),
            pltpu.VMEM((toks, d_model), BF16),
        ],
        compiler_params=pltpu.CompilerParams(vmem_limit_bytes=48 * 1024 * 1024),
        name="latent_attention",
    )(order, sorted_len, place.reshape(1, toks), x, cache_t, w_q, w_o)


MESH_ID = pl.DeviceIdType.MESH
EXP_STEP = 4


def moe_kernel(layer, x_ref, g_ref, ids_ref, slot_ref, gate_ref, w1, w3, w2, w1s, w3s, w2s, out_ref,
               gall, wall, route_ref, w2t, acc, part, gsend, grecv, rsend, rrecv, psend, precv):
    me = lax.axis_index('dp')
    core = lax.rem(me, 2)
    chip = lax.div(me, 2)
    partner = chip * 2 + (1 - core)
    cross = (1 - chip) * 2 + (1 - core)
    same = (1 - chip) * 2 + core
    peers = (partner, cross, same)
    _, experts, ff, d_model = w2.shape
    toks = x_ref.shape[0]

    expert_id = lax.broadcasted_iota(jnp.int32, route_ref.shape, 0)
    route = jnp.zeros(route_ref.shape, F32)
    for j in range(ids_ref.shape[0]):
        hit = (ids_ref[j, layer:layer + 1, :] == expert_id) & (slot_ref[j, layer:layer + 1, :] >= 0)
        route = route + jnp.where(hit, gate_ref[j, layer:layer + 1, :], 0.0)
    route_ref[...] = route

    barrier = pltpu.get_barrier_semaphore()
    for p in peers:
        pl.semaphore_signal(barrier, inc=1, device_id={'dp': p}, device_id_type=MESH_ID)
    pl.semaphore_wait(barrier, 3)

    gcopies, rcopies = [], []
    for i, p in enumerate(peers):
        rcopies.append(pltpu.make_async_remote_copy(
            route_ref.at[pl.ds(p * experts, experts)], wall.at[i + 1], rsend.at[i], rrecv.at[i],
            device_id={'dp': p}, device_id_type=MESH_ID))
        gcopies.append(pltpu.make_async_remote_copy(
            g_ref, gall.at[i + 1], gsend.at[i], grecv.at[i], device_id={'dp': p}, device_id_type=MESH_ID))
    for i in range(3):
        rcopies[i].start()
        gcopies[i].start()

    gall[0] = g_ref[...]
    wall[0] = route_ref[pl.ds(pl.multiple_of(me * experts, experts), experts), :]

    def flip(e, carry):
        w2t[e] = w2[layer, e].T
        return carry
    lax.fori_loop(0, experts, flip, 0)
    w2st = w2s[layer].T

    def gated(w3_rows, w1_rows, tok):
        dims = (((1,), (1,)), ((), ()))
        gate = lax.dot_general(w3_rows, tok, dims, preferred_element_type=F32)
        up = lax.dot_general(w1_rows, tok, dims, preferred_element_type=F32)
        return (gate * (1.0 / (1.0 + jnp.exp(-gate))) * up).astype(BF16)

    def ffn(blocks):
        tok = jnp.concatenate([gall[b] for b in blocks], axis=0)
        first = jnp.dot(w2st, gated(w3s[layer], w1s[layer], tok), preferred_element_type=F32)
        for n, b in enumerate(blocks):
            acc[b] = first[:, n * toks:(n + 1) * toks]

        def step(s, carry):
            rows = slice(s * EXP_STEP * ff, (s + 1) * EXP_STEP * ff)
            hid = gated(w3[layer, rows, :], w1[layer, rows, :], tok)
            total = [acc[b] for b in blocks]
            for i in range(EXP_STEP):
                e = s * EXP_STEP + i
                u = jnp.dot(w2t[e], hid[i * ff:(i + 1) * ff], preferred_element_type=F32)
                u = u.astype(BF16).astype(F32)
                for n, b in enumerate(blocks):
                    w = wall[b, e:e + 1, :]
                    total[n] = total[n] + jnp.where(w > 0.0, u[:, n * toks:(n + 1) * toks] * w, 0.0)
            for n, b in enumerate(blocks):
                acc[b] = total[n]
            return carry
        for s in range(experts // EXP_STEP):
            step(s, 0)

    def send_part(i, src, dst_ref, dst):
        return pltpu.make_async_remote_copy(
            src, dst_ref, psend.at[i], precv.at[i], device_id={'dp': dst}, device_id_type=MESH_ID)

    rcopies[1].wait_recv()
    gcopies[1].wait_recv()
    ffn((2,))
    relay = send_part(1, acc.at[2], part.at[1], partner)
    relay.start()

    rcopies[2].wait_recv()
    gcopies[2].wait_recv()
    ffn((3,))
    relay.wait_recv()
    half = d_model // 2
    far = []
    for i in range(2):
        rows = slice(i * half, (i + 1) * half)
        acc[4, rows] = acc[3, rows] + part[1, rows]
        at = pl.ds(i * half, half)
        far.append(send_part(2 + i, acc.at[4, at], part.at[2, at], same))
        far[i].start()

    rcopies[0].wait_recv()
    gcopies[0].wait_recv()
    ffn((0, 1))
    home = send_part(0, acc.at[1], part.at[0], partner)
    home.start()
    home.wait_recv()
    acc[0] = acc[0] + part[0]
    for i in range(2):
        rows = slice(i * half, (i + 1) * half)
        far[i].wait_recv()
        out_ref[:, rows] = (x_ref[:, rows].astype(F32) + (acc[0, rows] + part[2, rows]).T).astype(BF16)

    for c in gcopies + rcopies + [home, relay] + far:
        c.wait_send()


def moe(layer, x, g, ids, slot, gate, total_experts, w1, w3, w2, w1s, w3s, w2s):
    toks, d_model = x.shape
    _, experts, ff, _ = w2.shape
    vmem = pl.BlockSpec(memory_space=pltpu.VMEM)
    dma = pltpu.SemaphoreType.DMA
    return pl.pallas_call(
        functools.partial(moe_kernel, layer),
        out_shape=jax.ShapeDtypeStruct((toks, d_model), BF16),
        in_specs=[vmem] * 11,
        out_specs=vmem,
        scratch_shapes=[
            pltpu.VMEM((4, toks, d_model), BF16),
            pltpu.VMEM((4, experts, toks), F32),
            pltpu.VMEM((total_experts, toks), F32),
            pltpu.VMEM((experts, d_model, ff), BF16),
            pltpu.VMEM((5, d_model, toks), F32),
            pltpu.VMEM((3, d_model, toks), F32),
            dma((3,)), dma((3,)), dma((3,)), dma((3,)), dma((4,)), dma((4,)),
        ],
        compiler_params=pltpu.CompilerParams(
            collective_id=layer, has_side_effects=True, vmem_limit_bytes=40 * 1024 * 1024),
        name="expert_exchange",
    )(x, g, ids, slot, gate, w1, w3, w2, w1s, w3s, w2s)


def solution(mesh):
    tok_axes = ('replica', 'dp')
    in_specs = (
        P(tok_axes, None), P(tok_axes), P(None, tok_axes, None, None),
        P(None, None, None), P(None, None, None),
        P(None, tok_axes, None), P(None, tok_axes, None), P(None, tok_axes, None),
        P(None, 'dp', None, None), P(None, 'dp', None, None), P(None, 'dp', None, None),
        P(None, None, 'dp'), P(None, None, 'dp'), P(None, 'dp', None),
    )

    def device_step(x, lengths, cache, w_q, w_o, expert_ids, slots, route_w, w1_exp, w3_exp, w2_exp, w1_sh, w3_sh, w2_sh):
        layers, local, d_model, ff = w1_exp.shape
        place, order, sorted_len = bucket_order(lengths)
        cache_t = jnp.swapaxes(cache, 2, 3)
        by_choice = [jnp.transpose(a, (2, 0, 1)) for a in (expert_ids, slots, route_w)]
        w1 = jnp.swapaxes(w1_exp, 2, 3).reshape(layers, local * ff, d_model)
        w3 = jnp.swapaxes(w3_exp, 2, 3).reshape(layers, local * ff, d_model)
        w1s, w3s = jnp.swapaxes(w1_sh, 1, 2), jnp.swapaxes(w3_sh, 1, 2)
        experts = local * mesh.shape['dp']
        resid = x
        for layer in range(layers):
            resid, ffn_in = attention(layer, place, order, sorted_len, resid, cache_t, w_q, w_o)
            resid = moe(layer, resid, ffn_in, *by_choice, experts, w1, w3, w2_exp, w1s, w3s, w2_sh)
        return resid

    return jax.shard_map(device_step, mesh=mesh, in_specs=in_specs, out_specs=P(tok_axes, None), check_vma=False)
```

```python
import functools
import jax
import jax.numpy as jnp
from jax import lax
from jax.experimental import pallas as pl
from jax.experimental.pallas import tpu as pltpu
from jax.sharding import PartitionSpec as P

NORM_EPS = 1e-6
ATT_SCALE = 1.0 / (192.0 ** 0.5)
LATENT = 512
CHUNK = 128
F32 = jnp.float32
MXU_COLS = (512, 384, 256, 256)
VBLK = 64
BF16 = jnp.bfloat16


def rms_norm(values):
    vals32 = values.astype(F32)
    return vals32 * lax.rsqrt(jnp.mean(vals32 * vals32, axis=-1, keepdims=True) + NORM_EPS)


def bucket_order(lengths):
    count = lengths.shape[0]
    chunks = (lengths + (CHUNK - 1)) // CHUNK
    ids = jnp.arange(count, dtype=jnp.int32)
    ahead = (chunks[None, :] > chunks[:, None]) | ((chunks[None, :] == chunks[:, None]) & (ids[None, :] < ids[:, None]))
    place = jnp.sum(ahead.astype(jnp.int32), axis=1)
    hit = place[None, :] == ids[:, None]
    order = jnp.sum(jnp.where(hit, ids[None, :], 0), axis=1)
    sorted_len = jnp.sum(jnp.where(hit, lengths[None, :], 0), axis=1)
    return place, order, sorted_len


def attn_kernel(layer, slots, order_ref, slen_ref, place_ref, x_in, cache_ref, wq_hbm, wo_hbm,
                x_out, g_out, wq, wo, buf, qbd, obuf, pbuf, sem, wsem, xbuf):
    toks, d_model = x_in.shape
    kv_dim, seq_len = cache_ref.shape[2], cache_ref.shape[3]
    groups = toks // 8
    max_n = seq_len // CHUNK

    def group_n(g):
        return lax.div(slen_ref[g * 8] + (CHUNK - 1), CHUNK)

    def start_group(g):
        slot = lax.rem(g, slots)
        n = group_n(g)
        for nn in range(1, max_n + 1):
            @pl.when(n == nn)
            def _():
                cols = pl.ds(0, nn * CHUNK)
                for i in range(8):
                    b = order_ref[g * 8 + i]
                    pltpu.make_async_copy(
                        cache_ref.at[layer, b, :, cols],
                        buf.at[slot, i // 4, pl.ds((i % 4) * kv_dim, kv_dim), cols], sem.at[slot]).start()

    wq_copy = pltpu.make_async_copy(wq_hbm.at[layer], wq, wsem.at[0])
    wo_copy = pltpu.make_async_copy(wo_hbm.at[layer], wo, wsem.at[1])
    wq_copy.start()
    x_copy = pltpu.make_async_copy(x_in, xbuf, wsem.at[2])
    if layer == 0:
        x_copy.start()
    x_ref = xbuf if layer == 0 else x_in
    lax.fori_loop(0, slots, lambda g, c: (start_group(g), c)[1], 0)
    wo_copy.start()

    rows = 2 * toks
    row_id = lax.broadcasted_iota(jnp.int32, (rows, toks), 0)
    place = place_ref[...]
    base = lax.shift_right_logical(place, 2) * 8 + lax.rem(place, 4)
    pick0 = (row_id == base).astype(BF16)
    pick1 = (row_id == base + 4).astype(BF16)
    if layer == 0:
        x_copy.wait()
    h = rms_norm(x_ref[...]).astype(BF16)
    wq_copy.wait()
    q = jnp.dot(h, wq[...], preferred_element_type=F32).astype(BF16)
    qrows = (jnp.dot(pick0, q[:, :kv_dim], preferred_element_type=F32)
             + jnp.dot(pick1, q[:, kv_dim:], preferred_element_type=F32))
    sub = lax.rem(lax.broadcasted_iota(jnp.int32, (rows, 1), 0), 4)
    twice = jnp.concatenate([qrows, qrows], axis=1)
    second = (lax.broadcasted_iota(jnp.int32, (rows, 2 * kv_dim), 1) >= kv_dim).astype(jnp.int32)
    for jj in range(2):
        lhs = jnp.where(sub == 2 * jj + second, twice, 0.0).astype(BF16)
        for t in range(2 * kv_dim // CHUNK):
            qbd[jj * (2 * kv_dim // CHUNK) + t] = lhs[:, t * CHUNK:(t + 1) * CHUNK]

    row16 = lax.broadcasted_iota(jnp.int32, (16, CHUNK), 0)
    sub16 = lax.rem(row16, 4)
    lane16 = lax.broadcasted_iota(jnp.int32, (16, CHUNK), 1)
    half16 = (row16 >= 8).astype(jnp.int32)
    seq16 = half16 * 4 + sub16

    def scores(g, nn):
        slot = lax.rem(g, slots)
        at16 = pl.ds(pl.multiple_of(g * 16, 16), 16)
        lhs = jnp.concatenate([qbd[t, at16, :] for t in range(qbd.shape[0])], axis=1)
        lens = jnp.zeros((16, CHUNK), jnp.int32)
        for i in range(8):
            lens = jnp.where(seq16 == i, slen_ref[g * 8 + i], lens)
        out = []
        for k in range(nn):
            cols = pl.ds(k * CHUNK, CHUNK)
            rhs = jnp.concatenate([buf[slot, 0, :, cols], buf[slot, 1, :, cols]], axis=1)
            raw = jnp.dot(lhs, rhs, preferred_element_type=F32)
            s = jnp.concatenate([raw[0:8, :CHUNK], raw[8:16, CHUNK:]], axis=0) * ATT_SCALE
            out.append(jnp.where(lane16 + k * CHUNK < lens, s, -jnp.inf))
        return out

    def softmax(s):
        m = s[0]
        for t in s[1:]:
            m = jnp.maximum(m, t)
        m = jnp.max(m, axis=1, keepdims=True)
        e = [jnp.exp(t - m) for t in s]
        tot = e[0]
        for t in e[1:]:
            tot = tot + t
        inv = 1.0 / jnp.sum(tot, axis=1, keepdims=True)
        return [(t * inv) for t in e]

    lane_blk = lax.broadcasted_iota(jnp.int32, (VBLK, CHUNK), 1)

    def values(g, p):
        slot = lax.rem(g, slots)
        at16 = pl.ds(pl.multiple_of(g * 16, 16), 16)
        mxu_cols = MXU_COLS[len(p) - 1]
        lhs, rhs = [], []
        for k, t in enumerate(p):
            for j in range(4):
                for half in range(2):
                    keep = (sub16 == j) & (half16 == half)
                    lhs.append(jnp.where(keep, t, 0.0).astype(BF16))
                    rhs.append(buf[slot, half, pl.ds(j * kv_dim, mxu_cols), pl.ds(k * CHUNK, CHUNK)])
        o = lax.dot_general(jnp.concatenate(lhs, axis=1), jnp.concatenate(rhs, axis=1),
                            (((1,), (1,)), ((), ())), preferred_element_type=F32)
        obuf[at16, :mxu_cols] = o.astype(BF16)
        if mxu_cols == LATENT:
            return
        rounded = [t.astype(BF16).astype(F32) for t in p]
        blocks = (LATENT - mxu_cols) // VBLK
        picked = [jnp.zeros((VBLK, CHUNK), F32) for _ in range(blocks)]
        for half in range(2):
            for j in range(4):
                for c in range(blocks):
                    sums = [None, None]
                    for k in range(len(p)):
                        tile = buf[slot, half, pl.ds(j * kv_dim + mxu_cols + c * VBLK, VBLK), pl.ds(k * CHUNK, CHUNK)].astype(F32)
                        for head in range(2):
                            row = half * 8 + head * 4 + j
                            term = tile * rounded[k][row:row + 1, :]
                            sums[head] = term if k == 0 else sums[head] + term
                    for head in range(2):
                        row = half * 8 + head * 4 + j
                        picked[c] = jnp.where(lane_blk == row, jnp.sum(sums[head], axis=1, keepdims=True), picked[c])
        obuf[at16, mxu_cols:] = jnp.concatenate(picked, axis=0).T[:16].astype(BF16)

    def wait_group(g, nn):
        slot = lax.rem(g, slots)
        view = buf.at[slot, :, :, pl.ds(0, nn * CHUNK)]
        pltpu.make_async_copy(view, view, sem.at[slot]).wait()

    def put_scores(g, nn):
        for k, t in enumerate(scores(g, nn)):
            pbuf[lax.rem(g, 2), k] = t

    def put_values(g, nn):
        values(g, softmax([pbuf[lax.rem(g, 2), k] for k in range(nn)]))

    def each_n(n, fn):
        for nn in range(1, max_n + 1):
            pl.when(n == nn)(functools.partial(fn, nn))

    def first(nn):
        wait_group(0, nn)
    each_n(group_n(0), first)
    put_scores(0, max_n)

    def body(g, _):
        each_n(group_n(g), functools.partial(wait_group, g))

        def both(nn):
            raw_prev = [pbuf[lax.rem(g - 1, 2), k] for k in range(nn)]
            s = scores(g, nn)
            values(g - 1, softmax(raw_prev))
            for k, t in enumerate(s):
                pbuf[lax.rem(g, 2), k] = t
        each_n(group_n(g - 1), both)

        @pl.when(g - 1 + slots < groups)
        def _():
            start_group(g - 1 + slots)
        return 0

    lax.fori_loop(1, groups, body, 0)
    each_n(group_n(groups - 1), functools.partial(put_values, groups - 1))

    wo_copy.wait()
    picked = obuf[...]
    total = x_ref[...].astype(F32)
    for head, pick in enumerate((pick0, pick1)):
        o = lax.dot_general(pick, picked, (((0,), (0,)), ((), ())), preferred_element_type=F32).astype(BF16)
        total = total + jnp.dot(o, wo[head * LATENT:(head + 1) * LATENT, :], preferred_element_type=F32)
    x_new = total.astype(BF16)
    x_out[...] = x_new
    g_out[...] = rms_norm(x_new).astype(BF16)


def attention(layer, place, order, sorted_len, x, cache_t, w_q, w_o, slots=8):
    toks, d_model = x.shape
    kv_dim, seq_len = cache_t.shape[2], cache_t.shape[3]
    any_spec = pl.BlockSpec(memory_space=pltpu.HBM)
    if layer == 0:
        x, w_q, w_o = (pltpu.with_memory_space_constraint(a, pltpu.HBM) for a in (x, w_q, w_o))
    smem = pl.BlockSpec(memory_space=pltpu.SMEM)
    vmem = pl.BlockSpec(memory_space=pltpu.VMEM)
    return pl.pallas_call(
        functools.partial(attn_kernel, layer, slots),
        out_shape=(jax.ShapeDtypeStruct((toks, d_model), BF16), jax.ShapeDtypeStruct((toks, d_model), BF16)),
        in_specs=[smem, smem, vmem, any_spec if layer == 0 else vmem, any_spec, any_spec, any_spec],
        out_specs=(vmem, vmem),
        scratch_shapes=[
            pltpu.VMEM(w_q.shape[1:], BF16),
            pltpu.VMEM(w_o.shape[1:], BF16),
            pltpu.VMEM((slots, 2, 4 * kv_dim, seq_len), BF16),
            pltpu.VMEM((4 * kv_dim // CHUNK, 2 * toks, CHUNK), BF16),
            pltpu.VMEM((2 * toks, LATENT), BF16),
            pltpu.VMEM((2, seq_len // CHUNK, 16, CHUNK), F32),
            pltpu.SemaphoreType.DMA((slots,)),
            pltpu.SemaphoreType.DMA((3,)),
            pltpu.VMEM((toks, d_model), BF16),
        ],
        compiler_params=pltpu.CompilerParams(vmem_limit_bytes=48 * 1024 * 1024),
        name="latent_attention",
    )(order, sorted_len, place.reshape(1, toks), x, cache_t, w_q, w_o)


MESH_ID = pl.DeviceIdType.MESH
EXP_STEP = 8


def moe_kernel(layer, x_ref, g_ref, ids_ref, slot_ref, gate_ref, w1, w3, w2, w1s, w3s, w2s, out_ref,
               gall, wall, route_ref, w2t, acc, part, gsend, grecv, rsend, rrecv, psend, precv):
    me = lax.axis_index('dp')
    core = lax.rem(me, 2)
    chip = lax.div(me, 2)
    partner = chip * 2 + (1 - core)
    cross = (1 - chip) * 2 + (1 - core)
    same = (1 - chip) * 2 + core
    peers = (partner, cross, same)
    _, experts, ff, d_model = w2.shape
    toks = x_ref.shape[0]

    barrier = pltpu.get_barrier_semaphore()
    for p in peers:
        pl.semaphore_signal(barrier, inc=1, device_id={'dp': p}, device_id_type=MESH_ID)
    expert_id = lax.broadcasted_iota(jnp.int32, route_ref.shape, 0)
    route = jnp.zeros(route_ref.shape, F32)
    for j in range(ids_ref.shape[0]):
        hit = (ids_ref[j, layer:layer + 1, :] == expert_id) & (slot_ref[j, layer:layer + 1, :] >= 0)
        route = route + jnp.where(hit, gate_ref[j, layer:layer + 1, :], 0.0)
    route_ref[...] = route
    pl.semaphore_wait(barrier, 3)

    gcopies, rcopies = [], []
    for i, p in enumerate(peers):
        rcopies.append(pltpu.make_async_remote_copy(
            route_ref.at[pl.ds(p * experts, experts)], wall.at[i + 1], rsend.at[i], rrecv.at[i],
            device_id={'dp': p}, device_id_type=MESH_ID))
        gcopies.append(pltpu.make_async_remote_copy(
            g_ref, gall.at[i + 1], gsend.at[i], grecv.at[i], device_id={'dp': p}, device_id_type=MESH_ID))
    for i in range(3):
        rcopies[i].start()
        gcopies[i].start()

    gall[0] = g_ref[...]
    wall[0] = route_ref[pl.ds(pl.multiple_of(me * experts, experts), experts), :]

    def flip(e, carry):
        w2t[e] = w2[layer, e].T
        return carry
    lax.fori_loop(0, experts, flip, 0)
    w2st = w2s[layer].T

    def gated(w3_rows, w1_rows, tok):
        dims = (((1,), (1,)), ((), ()))
        gate = lax.dot_general(w3_rows, tok, dims, preferred_element_type=F32)
        up = lax.dot_general(w1_rows, tok, dims, preferred_element_type=F32)
        return (gate * (1.0 / (1.0 + jnp.exp(-gate))) * up).astype(BF16)

    def ffn(blocks):
        tok = jnp.concatenate([gall[b] for b in blocks], axis=0)
        first = jnp.dot(w2st, gated(w3s[layer], w1s[layer], tok), preferred_element_type=F32)
        for n, b in enumerate(blocks):
            acc[b] = first[:, n * toks:(n + 1) * toks]

        def step(s, carry):
            rows = slice(s * EXP_STEP * ff, (s + 1) * EXP_STEP * ff)
            hid = gated(w3[layer, rows, :], w1[layer, rows, :], tok)
            total = [acc[b] for b in blocks]
            for i in range(EXP_STEP):
                e = s * EXP_STEP + i
                u = jnp.dot(w2t[e], hid[i * ff:(i + 1) * ff], preferred_element_type=F32)
                u = u.astype(BF16).astype(F32)
                for n, b in enumerate(blocks):
                    w = wall[b, e:e + 1, :]
                    total[n] = total[n] + jnp.where(w > 0.0, u[:, n * toks:(n + 1) * toks] * w, 0.0)
            for n, b in enumerate(blocks):
                acc[b] = total[n]
            return carry
        for s in range(experts // EXP_STEP):
            step(s, 0)

    def send_part(i, src, dst_ref, dst):
        return pltpu.make_async_remote_copy(
            src, dst_ref, psend.at[i], precv.at[i], device_id={'dp': dst}, device_id_type=MESH_ID)

    rcopies[1].wait_recv()
    gcopies[1].wait_recv()
    ffn((2,))
    relay = send_part(1, acc.at[2], part.at[1], partner)
    relay.start()

    rcopies[2].wait_recv()
    gcopies[2].wait_recv()
    ffn((3,))
    relay.wait_recv()
    half = d_model // 2
    far = []
    for i in range(2):
        rows = slice(i * half, (i + 1) * half)
        acc[4, rows] = acc[3, rows] + part[1, rows]
        at = pl.ds(i * half, half)
        far.append(send_part(2 + i, acc.at[4, at], part.at[2, at], same))
        far[i].start()

    rcopies[0].wait_recv()
    gcopies[0].wait_recv()
    ffn((0, 1))
    home = send_part(0, acc.at[1], part.at[0], partner)
    home.start()
    home.wait_recv()
    acc[0] = acc[0] + part[0]
    for i in range(2):
        rows = slice(i * half, (i + 1) * half)
        far[i].wait_recv()
        out_ref[:, rows] = (x_ref[:, rows].astype(F32) + (acc[0, rows] + part[2, rows]).T).astype(BF16)

    for c in gcopies + rcopies + [home, relay] + far:
        c.wait_send()


def moe(layer, x, g, ids, slot, gate, total_experts, w1, w3, w2, w1s, w3s, w2s):
    toks, d_model = x.shape
    _, experts, ff, _ = w2.shape
    vmem = pl.BlockSpec(memory_space=pltpu.VMEM)
    dma = pltpu.SemaphoreType.DMA
    return pl.pallas_call(
        functools.partial(moe_kernel, layer),
        out_shape=jax.ShapeDtypeStruct((toks, d_model), BF16),
        in_specs=[vmem] * 11,
        out_specs=vmem,
        scratch_shapes=[
            pltpu.VMEM((4, toks, d_model), BF16),
            pltpu.VMEM((4, experts, toks), F32),
            pltpu.VMEM((total_experts, toks), F32),
            pltpu.VMEM((experts, d_model, ff), BF16),
            pltpu.VMEM((5, d_model, toks), F32),
            pltpu.VMEM((3, d_model, toks), F32),
            dma((3,)), dma((3,)), dma((3,)), dma((3,)), dma((4,)), dma((4,)),
        ],
        compiler_params=pltpu.CompilerParams(
            collective_id=layer, has_side_effects=True, vmem_limit_bytes=40 * 1024 * 1024),
        name="expert_exchange",
    )(x, g, ids, slot, gate, w1, w3, w2, w1s, w3s, w2s)


def solution(mesh):
    tok_axes = ('replica', 'dp')
    in_specs = (
        P(tok_axes, None), P(tok_axes), P(None, tok_axes, None, None),
        P(None, None, None), P(None, None, None),
        P(None, tok_axes, None), P(None, tok_axes, None), P(None, tok_axes, None),
        P(None, 'dp', None, None), P(None, 'dp', None, None), P(None, 'dp', None, None),
        P(None, None, 'dp'), P(None, None, 'dp'), P(None, 'dp', None),
    )

    def device_step(x, lengths, cache, w_q, w_o, expert_ids, slots, route_w, w1_exp, w3_exp, w2_exp, w1_sh, w3_sh, w2_sh):
        layers, local, d_model, ff = w1_exp.shape
        place, order, sorted_len = bucket_order(lengths)
        cache_t = jnp.swapaxes(cache, 2, 3)
        by_choice = [jnp.transpose(a, (2, 0, 1)) for a in (expert_ids, slots, route_w)]
        w1 = jnp.swapaxes(w1_exp, 2, 3).reshape(layers, local * ff, d_model)
        w3 = jnp.swapaxes(w3_exp, 2, 3).reshape(layers, local * ff, d_model)
        w1s, w3s = jnp.swapaxes(w1_sh, 1, 2), jnp.swapaxes(w3_sh, 1, 2)
        experts = local * mesh.shape['dp']
        resid = x
        for layer in range(layers):
            resid, ffn_in = attention(layer, place, order, sorted_len, resid, cache_t, w_q, w_o)
            resid = moe(layer, resid, ffn_in, *by_choice, experts, w1, w3, w2_exp, w1s, w3s, w2_sh)
        return resid

    return jax.shard_map(device_step, mesh=mesh, in_specs=in_specs, out_specs=P(tok_axes, None), check_vma=False)
```
